32 devices in a mesh: grp: 2 (over y), pulse: 4 (over z), chan: 2 (over x), sub: 2 (over core).
Axes of the slice: x: 2, y: 2, z: 4, core: 2. Of those that a mesh axis runs over, the one named last changes fastest.
Arguments:
- samples: int32 [2, 16, 512, 4096], P(None, ('grp', 'chan', 'sub'), 'pulse'), parts along dimension 1, may hold values from -2048 to 2047
- replica: float32 [2, 4096], replicated, may hold values from -6 to 6
- window: int32 [16, 2], P(('grp', 'chan', 'sub')), parts along dimension 0, may hold values from 1 to 28, as said below
- thresh: int32 [16, 2], P(('grp', 'chan', 'sub')), parts along dimension 0, may hold values from 2 to 32, as said below
Outputs:
- ratio_map: float32 [16, 512, 4096], P(('grp', 'chan', 'sub'), None, 'pulse'), parts along dimension 0
- detections: float32 [2], P('grp'), parts along dimension 0
The draws below stay inside these ranges and needn't reach their ends.
There are 2 independent parts, one for each index of `grp`. The reference program is written for one: setup_inputs(seed, part) draws one part's arguments, and reference() takes and returns one part's arrays. A program takes and returns all parts, laid end to end along the dimension named above; an argument that names none is the same for every part. Nothing has to cross between parts.
Inputs may be any that keep to these rules, and one draw needn't show every extreme that they name: `window`: column 0 is a channel's guard gates on each side, 1 to 4; column 1 its training gates on each side, 14 to 28; some channel has both at their most. `thresh`: column 0 is a numerator of 8 to 32, column 1 a denominator of 2 to 4.
All inputs are finite; a program needn't handle non-finite values.
Results may differ from the reference program's by a relative error of at most 0.0003.
Values sent between devices are 32-bit elements; how exact they have to be, the bound alone decides.
A program may use at most 128 MiB of HBM per device.

```python
import jax
import jax.numpy as jnp
from jax import lax

PULSES = 512
RANGE = 4096
GUARD_MAX = 4
TRAIN_MAX = 28
CHANNELS = 8


def draw_window(key, part):
    guard_key, train_key, pick_key = jax.random.split(jax.random.fold_in(key, 11), 3)
    guards = jax.random.randint(guard_key, (CHANNELS,), 1, GUARD_MAX + 1)
    trains = jax.random.randint(train_key, (CHANNELS,), TRAIN_MAX // 2, TRAIN_MAX + 1)
    chosen = jax.random.randint(pick_key, (), 0, CHANNELS)
    is_pick = jnp.arange(CHANNELS) == chosen
    guards = jnp.where(is_pick, GUARD_MAX, guards)
    trains = jnp.where(is_pick, TRAIN_MAX, trains)
    return jnp.stack([guards, trains], axis=1).astype(jnp.int32)


def draw_thresh(key, part):
    num_key, den_key = jax.random.split(jax.random.fold_in(key, 23))
    numerators = jax.random.randint(num_key, (CHANNELS,), 8, 33)
    denominators = jax.random.randint(den_key, (CHANNELS,), 2, 5)
    return jnp.stack([numerators, denominators], axis=1).astype(jnp.int32)


def with_ends(array, rng, least, top_value):
    longest = array.shape.index(max(array.shape))
    spots = []
    for shift in (0, 1):
        where = [jax.random.randint(jax.random.fold_in(rng, axis), (), 0, length) for axis, length in enumerate(array.shape)]
        where[longest] = (where[longest] + shift) % array.shape[longest]
        spots.append(tuple(where))
    return array.at[spots[0]].set(least).at[spots[1]].set(top_value)


def gaussian(key, shape, spread, bound, kind=jnp.bfloat16):
    array = jax.random.normal(key, shape, jnp.float32) * spread
    return jnp.minimum(jnp.maximum(array, -bound), bound).astype(kind)


def setup_inputs(seed: int = 0, part: int = 0) -> dict:
    key_of = jax.random.split(jax.random.key(seed), 5)
    own_keys = jax.random.split(jax.random.fold_in(key_of[4], part), 5)
    samples = with_ends(jax.random.randint(own_keys[0], (2, CHANNELS, PULSES, RANGE), -2048, 2048), jax.random.fold_in(own_keys[0], 1), -2048, 2047).astype(jnp.int32)
    replica = gaussian(key_of[1], (2, RANGE), 1.0, 6.0, jnp.float32)
    window = draw_window(jax.random.fold_in(jax.random.fold_in(key_of[4], part), 71), part)
    thresh = draw_thresh(jax.random.fold_in(jax.random.fold_in(key_of[4], part), 71), part)
    return {"samples": samples, "replica": replica, "window": window, "thresh": thresh}


def reference(samples, replica, window, thresh):
    margin = GUARD_MAX + TRAIN_MAX
    filt = lax.complex(replica[0], replica[1])

    def per_channel(index):
        chan_samples = lax.dynamic_index_in_dim(samples, index, 1, keepdims=False)
        chan_window = lax.dynamic_index_in_dim(window, index, 0, keepdims=False)
        chan_thresh = lax.dynamic_index_in_dim(thresh, index, 0, keepdims=False)
        signal = lax.complex(chan_samples[0].astype(jnp.float32) / 2048.0, chan_samples[1].astype(jnp.float32) / 2048.0)
        spectrum = jnp.fft.fft(signal, axis=-1, norm="ortho")
        compressed = jnp.fft.ifft(spectrum * filt[None, :], axis=-1, norm="ortho")
        doppler = jnp.fft.fft(compressed, axis=0, norm="ortho")
        power = jnp.real(doppler) ** 2 + jnp.imag(doppler) ** 2
        guard = chan_window[0]
        train = chan_window[1]
        padded = jnp.pad(power, ((0, 0), (margin, margin)))
        inside = jnp.pad(jnp.ones((RANGE,), jnp.float32), (margin, margin))
        noise_sum = jnp.zeros_like(power)
        cells = jnp.zeros((RANGE,), jnp.float32)
        for offset in range(1, margin + 1):
            weight = ((offset > guard) & (offset <= guard + train)).astype(jnp.float32)
            noise_sum = noise_sum + weight * (padded[:, margin + offset:margin + offset + RANGE] + padded[:, margin - offset:margin - offset + RANGE])
            cells = cells + weight * (inside[margin + offset:margin + offset + RANGE] + inside[margin - offset:margin - offset + RANGE])
        level = (noise_sum + 1e-6) / cells[None, :]
        ratio = power / level
        scale = chan_thresh[0].astype(jnp.float32) / chan_thresh[1].astype(jnp.float32)
        soft = jnp.clip(ratio / scale - 1.0, 0.0, 1.0)
        return ratio, jnp.sum(soft)

    ratio_map, soft_sums = lax.map(per_channel, jnp.arange(CHANNELS, dtype=jnp.int32))
    detections = jnp.sum(soft_sums) * (1024.0 / (PULSES * RANGE))
    return ratio_map, detections.reshape(1)
```

```python
import functools
import math

import jax
import jax.numpy as jnp
import numpy as np
from jax import lax
from jax.experimental import pallas as pl
from jax.experimental.pallas import tpu as pltpu
from jax.sharding import PartitionSpec as P

GUARD_MAX = 4
TRAIN_MAX = 28
MARGIN = GUARD_MAX + TRAIN_MAX
EPSILON = 1e-06
INPUT_SCALE = 1.0 / 2048.0
LANES = 128
SUB = 8
RADIX = 4


def halves(table):
    hi = np.asarray(table, np.float32).astype(jnp.bfloat16)
    lo = (np.asarray(table, np.float64) - hi.astype(np.float64)).astype(jnp.bfloat16)
    return hi, lo


MESH = pl.DeviceIdType.MESH
ROWS = 16
AHEAD = 3


def lane_table(sign):
    idx = np.arange(LANES)
    ang = 2.0 * np.pi * ((idx[:, None] * idx[None, :]) % LANES) / LANES
    c, s = np.cos(ang), sign * np.sin(ang)
    full = np.block([[c, s], [-s, c]])
    hi, lo = halves(full)
    return np.concatenate([hi, hi, lo], axis=0)


def doppler_table(pulses):
    part = pulses // RADIX
    m = np.arange(part)
    out = []
    for res in range(RADIX):
        ang = 2.0 * np.pi * ((m[None, :] * (RADIX * m[:, None] + res)) % pulses) / pulses
        c, s = np.cos(ang) / math.sqrt(pulses), -np.sin(ang) / math.sqrt(pulses)
        full = np.block([[c, -s], [s, c]])
        hi, lo = halves(full)
        out.append(np.concatenate([hi, hi, lo], axis=1))
    return np.stack(out)


def split(x, axis):
    hi = x.astype(jnp.bfloat16)
    lo = (x - hi.astype(jnp.float32)).astype(jnp.bfloat16)
    return jnp.concatenate([hi, lo, hi], axis=axis)


def fft_list(re, im, sign):
    n = len(re)
    if n == 1:
        return re, im
    er, ei = fft_list(re[0::2], im[0::2], sign)
    odd_r, odd_i = fft_list(re[1::2], im[1::2], sign)
    half = n // 2
    out_r, out_i = [None] * n, [None] * n
    for k in range(half):
        a, b = odd_r[k], odd_i[k]
        if k == 0:
            tr, ti = a, b
        elif 4 * k == n:
            tr, ti = (b, -a) if sign < 0 else (-b, a)
        elif 8 * k == n or 8 * k == 3 * n:
            h = math.sqrt(0.5)
            c = h if 8 * k == n else -h
            tr = c * a - (sign * h) * b
            ti = c * b + (sign * h) * a
        else:
            c = math.cos(2.0 * math.pi * k / n)
            s = sign * math.sin(2.0 * math.pi * k / n)
            tr = c * a - s * b
            ti = s * a + c * b
        out_r[k], out_i[k] = er[k] + tr, ei[k] + ti
        out_r[k + half], out_i[k + half] = er[k] - tr, ei[k] - ti
    return out_r, out_i


def range_rows(xs, c, r0, tw8, rep8, wf, wi, comp):
    n, per = comp.shape[1], comp.shape[2]
    cols = n * per
    rows = pl.ds(r0, SUB)
    re = [xs[0, c, rows, a * LANES:(a + 1) * LANES].astype(jnp.float32) for a in range(cols)]
    im = [xs[1, c, rows, a * LANES:(a + 1) * LANES].astype(jnp.float32) for a in range(cols)]
    re, im = fft_list(re, im, -1.0)
    mr, mi = jnp.concatenate(re, axis=0), jnp.concatenate(im, axis=0)
    tr, ti = tw8[0], tw8[1]
    m = jnp.concatenate([mr * tr - mi * ti, mr * ti + mi * tr], axis=1)
    f = jnp.dot(split(m, 1), wf[...], preferred_element_type=jnp.float32)
    fr, fi = f[:, :LANES], f[:, LANES:]
    tr, ti = rep8[0], rep8[1]
    m = jnp.concatenate([fr * tr - fi * ti, fr * ti + fi * tr], axis=1)
    f = jnp.dot(split(m, 1), wi[...], preferred_element_type=jnp.float32)
    fr, fi = f[:, :LANES], f[:, LANES:]
    tr, ti = tw8[0], tw8[1]
    mr, mi = fr * tr + fi * ti, fi * tr - fr * ti
    re = [mr[a * SUB:(a + 1) * SUB] for a in range(cols)]
    im = [mi[a * SUB:(a + 1) * SUB] for a in range(cols)]
    re, im = fft_list(re, im, 1.0)
    for j in range(n):
        for a in range(per):
            comp[c, j, a, 0, rows, :] = re[j * per + a]
            comp[c, j, a, 1, rows, :] = im[j * per + a]


def doppler_chunk(recv, c, g, table, pw, hi_ref, lo_ref):
    quarter = recv.shape[3] // RADIX
    a, b, cc, d = ([recv[c, g, ri, q * quarter:(q + 1) * quarter, :] for ri in range(2)] for q in range(RADIX))
    sr, si = a[0] + cc[0], a[1] + cc[1]
    dr, di = a[0] - cc[0], a[1] - cc[1]
    ur, ui = b[0] + d[0], b[1] + d[1]
    vr, vi = b[0] - d[0], b[1] - d[1]
    ys = [(sr + ur, si + ui), (dr + vi, di - vr), (sr - ur, si - ui), (dr - vi, di + vr)]
    for res in range(RADIX):
        y = jnp.concatenate(ys[res], axis=0)
        out = jnp.dot(table[res], split(y, 0), preferred_element_type=jnp.float32)
        re, im = out[:quarter], out[quarter:]
        p = re * re + im * im
        hi = p.astype(jnp.bfloat16)
        pw[c, g, res] = p
        hi_ref[c, g + 1, res] = hi
        lo_ref[c, g + 1, res] = (p - hi.astype(jnp.float32)).astype(jnp.bfloat16)


def cfar_chunk(c, g, first_gate, gates, thresh, window, pw, hi_ref, lo_ref, band, stage, acc):
    quarter = pw.shape[3]
    total = RADIX * quarter
    parts = [ref[c, g + k].reshape(total, LANES) for ref in (hi_ref, lo_ref) for k in range(3)]
    noise = jnp.dot(jnp.concatenate(parts, axis=1), band[c], preferred_element_type=jnp.float32)
    guard = window[c, 0]
    reach = guard + window[c, 1]
    gate = first_gate + g * LANES + lax.broadcasted_iota(jnp.int32, (SUB, LANES), 1)
    after = gates - 1 - gate
    cells = jnp.minimum(gate, reach) - jnp.minimum(gate, guard) + jnp.minimum(after, reach) - jnp.minimum(after, guard)
    cells = cells.astype(jnp.float32)[:1]
    inv = thresh[c, 1].astype(jnp.float32) / thresh[c, 0].astype(jnp.float32)
    ratio = pw[c, g].reshape(total, LANES) * cells / (noise + EPSILON)
    for res in range(RADIX):
        stage[c, g, pl.ds(res, quarter, stride=RADIX), :] = ratio[res * quarter:(res + 1) * quarter]
    soft = jnp.clip(ratio * inv - 1.0, 0.0, 1.0)
    acc[...] += jnp.sum(soft.reshape(total // SUB, SUB, LANES), axis=0)


def kernel(sizes, thresh, window, tw, rep, x_hbm, wf_hbm, wi_hbm, t_hbm, out_hbm, count,
           xs, wf, wi, table, tw8, rep8, comp, recv, pw, hi_ref, lo_ref, band, stage, pack, halo, gather, acc,
           in_sem, tab_sem, row_send, row_recv, chunk_send, chunk_recv, halo_send, halo_recv, out_sem, sum_sem):
    n, nx, ns, rows = sizes
    _, channels, part, gates = xs.shape
    chunks = comp.shape[2]
    quarter = pw.shape[3]
    pulses = RADIX * quarter
    own = gates // n
    blocks = part // rows
    last = channels - 1
    z, x, s = lax.axis_index("pulse"), lax.axis_index("chan"), lax.axis_index("sub")
    peers = n * nx * ns
    me = (z * nx + x) * ns + s
    h = n // 2
    half = z // h

    def peer(p):
        i = lax.rem(me + p, peers)
        return {"pulse": i // (nx * ns), "chan": lax.rem(i // ns, nx), "sub": lax.rem(i, ns)}

    barrier = pltpu.get_barrier_semaphore()

    def greet(p, carry):
        pl.semaphore_signal(barrier, 1, device_id=peer(p), device_id_type=MESH)
        return carry

    def load(b):
        c = b // blocks
        r = pl.ds(pl.multiple_of(lax.rem(b, blocks) * rows, rows), rows)
        return pltpu.make_async_copy(x_hbm.at[:, c, r, :], xs.at[:, c, r, :], in_sem.at[b])

    def start_load(b, carry):
        load(b).start()
        return carry

    tables = [pltpu.make_async_copy(a, b, tab_sem.at[i])
              for i, (a, b) in enumerate(((wf_hbm, wf), (wi_hbm, wi), (t_hbm, table)))]
    load(0).start()
    tables[0].start()
    tables[1].start()
    lax.fori_loop(1, channels * blocks, start_load, 0)
    tables[2].start()
    lax.fori_loop(1, peers, greet, 0)
    for k in range(tw.shape[1]):
        for ri in range(2):
            tw8[ri, k * SUB:(k + 1) * SUB, :] = jnp.broadcast_to(tw[ri, k:k + 1, :], (SUB, LANES))
            rep8[ri, k * SUB:(k + 1) * SUB, :] = jnp.broadcast_to(rep[ri, k:k + 1, :], (SUB, LANES))

    def near(k):
        return half * h + lax.rem(lax.rem(z, h) + 1 + k, h)

    def cross(k):
        return (1 - half) * h + lax.rem(z + s + k, h)

    def row_copy(c, dest, b):
        r = pl.multiple_of(b * rows, rows)
        return pltpu.make_async_remote_copy(
            comp.at[c, dest, :, :, pl.ds(r, rows), :],
            recv.at[c, :, :, pl.ds(pl.multiple_of(z * part + r, rows), rows), :],
            row_send.at[c, dest], row_recv.at[c, z],
            device_id={"pulse": dest}, device_id_type=MESH)

    def row_all(c, dest, src):
        return pltpu.make_async_remote_copy(
            comp.at[c, dest], recv.at[c, :, :, pl.ds(pl.multiple_of(src * part, part), part), :],
            row_send.at[c, dest], row_recv.at[c, src],
            device_id={"pulse": dest}, device_id_type=MESH)

    def chunk_copy(dest, src, g):
        return pltpu.make_async_remote_copy(
            comp.at[last, dest, g], recv.at[last, g, :, pl.ds(pl.multiple_of(src * part, part), part), :],
            chunk_send.at[dest, g], chunk_recv.at[src, g],
            device_id={"pulse": dest}, device_id_type=MESH)

    outer = jnp.logical_and(n == 4, jnp.logical_or(z == 0, z == n - 1))

    def row_near(c, b):
        for k in range(h - 1):
            row_copy(c, near(k), b).start()

    def row_cross(c, b):
        for k in range(h):
            row_copy(c, cross(k), b).start()

    def step(b, carry):
        c = b // blocks
        r0 = lax.rem(b, blocks) * rows
        load(b).wait()

        @pl.when(b == 0)
        def _():
            tables[0].wait()
            tables[1].wait()

        for u in range(rows // SUB):
            range_rows(xs, c, pl.multiple_of(r0 + u * SUB, SUB), tw8, rep8, wf, wi, comp)

        @pl.when(b == 1)
        def _():
            pl.semaphore_wait(barrier, peers - 1)

        @pl.when(jnp.logical_and(b >= 1, b <= last * blocks))
        def _():
            pc, pb = (b - 1) // blocks, lax.rem(b - 1, blocks)

            @pl.when(outer)
            def _():
                row_near(pc, pb)

            @pl.when(jnp.logical_not(outer))
            def _():
                row_cross(pc, pb)

        return carry

    lax.fori_loop(0, channels * blocks, step, 0)

    def each(body, lo, hi):
        def run(i, carry):
            body(i)
            return carry
        lax.fori_loop(lo, hi, run, 0)

    def order(k):
        odd = lax.rem(k, 2)
        return odd * (chunks - 1) + (1 - 2 * odd) * (k // 2)

    def rest(t):
        c, b = t // blocks, lax.rem(t, blocks)

        @pl.when(outer)
        def _():
            row_cross(c, b)

        @pl.when(jnp.logical_not(outer))
        def _():
            row_near(c, b)

    def last_near(k):
        for q in range(h - 1):
            chunk_copy(near(q), z, order(k)).start()

    def last_cross(k):
        for q in range(h):
            chunk_copy(cross(q), z, order(k)).start()

    ahead = min(AHEAD, chunks)
    each(last_near, 0, chunks)
    each(rest, 0, last * blocks)
    each(last_cross, 0, ahead)

    def keep(t):
        c, g = t // chunks, lax.rem(t, chunks)
        for ri in range(2):
            recv[c, g, ri, pl.ds(pl.multiple_of(z * part, part), part), :] = comp[c, z, g, ri]

    each(keep, 0, channels * chunks)
    q = lax.broadcasted_iota(jnp.int32, (3 * LANES, LANES), 0)
    j = lax.broadcasted_iota(jnp.int32, (3 * LANES, LANES), 1)
    dist = jnp.abs(q - LANES - j)
    for c in range(channels):
        guard = window[c, 0]
        reach = guard + window[c, 1]
        inside = jnp.where(dist > guard, 1.0, 0.0) * jnp.where(dist <= reach, 1.0, 0.0)
        inside = inside.astype(jnp.bfloat16)
        band[c] = jnp.concatenate([inside, inside], axis=0)
        blank = jnp.zeros((RADIX, quarter, LANES), jnp.bfloat16)
        for ref in (hi_ref, lo_ref):
            ref[c, 0] = blank
            ref[c, chunks + 1] = blank
    acc[...] = jnp.zeros_like(acc)
    tables[2].wait()

    def out_copy(c, g):
        lanes = pl.ds(pl.multiple_of(g * LANES, LANES), LANES)
        return pltpu.make_async_copy(stage.at[c, g], out_hbm.at[c, :, lanes], out_sem.at[c, g])

    def dop(c, g):
        doppler_chunk(recv, c, g, table, pw, hi_ref, lo_ref)

    def cfar(c, g):
        cfar_chunk(c, g, z * own, gates, thresh, window, pw, hi_ref, lo_ref, band, stage, acc)
        out_copy(c, g).start()

    def pack_left(c):
        pack[c, 0] = jnp.concatenate([pw[c, 0, res][:, :MARGIN] for res in range(RADIX)], axis=1)

    def pack_right(c):
        pack[c, 1] = jnp.concatenate([pw[c, chunks - 1, res][:, LANES - MARGIN:] for res in range(RADIX)], axis=1)

    def halo_copy(c, side, dest):
        return pltpu.make_async_remote_copy(
            pack.at[c, side], halo.at[c, 1 - side], halo_send.at[c, side], halo_recv.at[c, 1 - side],
            device_id={"pulse": dest}, device_id_type=MESH)

    def send_halo(c):
        @pl.when(z > 0)
        def _():
            halo_copy(c, 0, z - 1).start()

        @pl.when(z < n - 1)
        def _():
            halo_copy(c, 1, z + 1).start()

    def unpack(c, side):
        for res in range(RADIX):
            turn = (LANES - MARGIN - MARGIN * res if side == 0 else LANES - MARGIN * res) % LANES
            p = halo[c, side]
            if turn:
                p = pltpu.roll(p, turn, 1)
            hi = p.astype(jnp.bfloat16)
            at = 0 if side == 0 else chunks + 1
            hi_ref[c, at, res] = hi
            lo_ref[c, at, res] = (p - hi.astype(jnp.float32)).astype(jnp.bfloat16)

    def take_halo(c):
        @pl.when(z > 0)
        def _():
            halo_copy(c, 1, z).wait_recv()
            unpack(c, 0)

        @pl.when(z < n - 1)
        def _():
            halo_copy(c, 0, z).wait_recv()
            unpack(c, 1)

    for c in range(last):
        for o in range(1, n):
            row_all(c, z, lax.rem(z + o, n)).wait_recv()
        each(functools.partial(dop, c), 0, chunks)
        pack_left(c)
        pack_right(c)
        if chunks > 2:
            cfar(c, 1)
        send_halo(c)
        each(functools.partial(cfar, c), 2, chunks - 1)

    def arrive(k):
        for o in range(1, n):
            chunk_copy(z, lax.rem(z + o, n), order(k)).wait_recv()

    head = chunks - 1 if chunks >= 4 else chunks

    def last_step(k):
        @pl.when(k + ahead < chunks)
        def _():
            last_cross(k + ahead)

        arrive(k)
        dop(last, order(k))

        @pl.when(k == 0)
        def _():
            pack_left(last)

        @pl.when(k == min(1, chunks - 1))
        def _():
            pack_right(last)

        if chunks >= 4:
            @pl.when(k == 2)
            def _():
                send_halo(last)

            @pl.when(k >= 4)
            def _():
                cfar(last, order(k - 2))

    each(last_step, 0, head)
    if chunks < 4:
        send_halo(last)
        each(functools.partial(cfar, last), 1, chunks - 1)
    for c in range(channels):
        take_halo(c)
    edges = min(2, chunks)

    def edge(t):
        cfar(t // edges, lax.rem(t, edges) * (chunks - 1))

    each(edge, 0, channels * edges)
    if chunks >= 4:
        arrive(chunks - 1)
        dop(last, order(jnp.int32(chunks - 1)))
        each(lambda k: cfar(last, order(k)), chunks - 3, chunks)

    gather[me] = acc[...]
    for c in range(last):
        for o in range(1, n):
            row_all(c, lax.rem(z + o, n), z).wait_send()

    def sent(g):
        for o in range(1, n):
            chunk_copy(lax.rem(z + o, n), z, g).wait_send()

    each(sent, 0, chunks)
    for c in range(channels):
        @pl.when(z > 0)
        def _():
            halo_copy(c, 0, z - 1).wait_send()

        @pl.when(z < n - 1)
        def _():
            halo_copy(c, 1, z + 1).wait_send()

    def tell(p):
        pltpu.make_async_remote_copy(
            gather.at[me], gather.at[me], sum_sem.at[0], sum_sem.at[1],
            device_id=peer(p), device_id_type=MESH).start()

    each(tell, 1, peers)
    each(lambda t: out_copy(t // chunks, lax.rem(t, chunks)).wait(), 0, channels * chunks)
    every = pltpu.make_async_remote_copy(
        gather.at[pl.ds(0, peers - 1)], gather.at[pl.ds(0, peers - 1)], sum_sem.at[0], sum_sem.at[1],
        device_id=peer(1), device_id_type=MESH)
    every.wait()
    total = jnp.sum(gather[...], axis=0)
    count[0] = jnp.sum(total) * (1024.0 / (pulses * gates))


def local(samples, replica, window, thresh):
    _, channels, part, gates = samples.shape
    n, nx, ns = (lax.axis_size(a) for a in ("pulse", "chan", "sub"))
    cols = gates // LANES
    pulses = part * n
    own = gates // n
    chunks = own // LANES
    quarter = pulses // RADIX
    rows = min(ROWS, part)
    k1 = np.arange(cols)[:, None]
    b = np.arange(LANES)[None, :]
    ang = 2.0 * np.pi * ((k1 * b) % gates) / gates
    tw = np.stack([np.cos(ang), -np.sin(ang)]).astype(np.float32)
    rep = jnp.swapaxes(replica.reshape(2, LANES, cols), 1, 2) * (INPUT_SCALE / gates)
    wf, wi = lane_table(-1.0), lane_table(1.0)
    table = doppler_table(pulses)
    peers = n * nx * ns
    f32, bf16 = jnp.float32, jnp.bfloat16
    smem, vmem, hbm = (pl.BlockSpec(memory_space=m) for m in (pltpu.SMEM, pltpu.VMEM, pl.ANY))
    dma = pltpu.SemaphoreType.DMA
    return pl.pallas_call(
        functools.partial(kernel, (n, nx, ns, rows)),
        in_specs=[smem, smem, vmem, vmem, hbm, hbm, hbm, hbm],
        out_specs=[hbm, smem],
        out_shape=[jax.ShapeDtypeStruct((channels, pulses, own), f32), jax.ShapeDtypeStruct((1,), f32)],
        scratch_shapes=[
            pltpu.VMEM((2, channels, part, gates), jnp.int32),
            pltpu.VMEM(wf.shape, bf16),
            pltpu.VMEM(wi.shape, bf16),
            pltpu.VMEM(table.shape, bf16),
            pltpu.VMEM((2, cols * SUB, LANES), f32),
            pltpu.VMEM((2, cols * SUB, LANES), f32),
            pltpu.VMEM((channels, n, chunks, 2, part, LANES), f32),
            pltpu.VMEM((channels, chunks, 2, pulses, LANES), f32),
            pltpu.VMEM((channels, chunks, RADIX, quarter, LANES), f32),
            pltpu.VMEM((channels, chunks + 2, RADIX, quarter, LANES), bf16),
            pltpu.VMEM((channels, chunks + 2, RADIX, quarter, LANES), bf16),
            pltpu.VMEM((channels, 6 * LANES, LANES), bf16),
            pltpu.VMEM((channels, chunks, pulses, LANES), f32),
            pltpu.VMEM((channels, 2, quarter, LANES), f32),
            pltpu.VMEM((channels, 2, quarter, LANES), f32),
            pltpu.VMEM((peers, SUB, LANES), f32),
            pltpu.VMEM((SUB, LANES), f32),
            dma((channels * (part // rows),)),
            dma((3,)),
            dma((channels, n)),
            dma((channels, n)),
            dma((n, chunks)),
            dma((n, chunks)),
            dma((channels, 2)),
            dma((channels, 2)),
            dma((channels, chunks)),
            dma((2,)),
        ],
        compiler_params=pltpu.CompilerParams(
            collective_id=0, has_side_effects=True, vmem_limit_bytes=60 << 20),
        cost_estimate=pl.CostEstimate(flops=int(2e10), bytes_accessed=32 << 20, transcendentals=0),
    )(thresh, window, jnp.asarray(tw), rep, samples, jnp.asarray(wf), jnp.asarray(wi), jnp.asarray(table))


def solution(mesh):
    in_specs = (
        P(None, ("grp", "chan", "sub"), "pulse", None),
        P(),
        P(("grp", "chan", "sub"), None),
        P(("grp", "chan", "sub"), None),
    )
    out_specs = (P(("grp", "chan", "sub"), None, "pulse"), P("grp"))
    return jax.shard_map(lambda *a: tuple(local(*a)), mesh=mesh, in_specs=in_specs, out_specs=out_specs, check_vma=False)
```

```python
import functools
import math

import jax
import jax.numpy as jnp
import numpy as np
from jax import lax
from jax.experimental import pallas as pl
from jax.experimental.pallas import tpu as pltpu
from jax.sharding import PartitionSpec as P

GUARD_MAX = 4
TRAIN_MAX = 28
MARGIN = GUARD_MAX + TRAIN_MAX
EPSILON = 1e-06
INPUT_SCALE = 1.0 / 2048.0
LANES = 128
SUB = 8
RADIX = 4


def halves(table):
    hi = np.asarray(table, np.float32).astype(jnp.bfloat16)
    lo = (np.asarray(table, np.float64) - hi.astype(np.float64)).astype(jnp.bfloat16)
    return hi, lo


MESH = pl.DeviceIdType.MESH
ROWS = 16
AHEAD = 3


def lane_table(sign):
    idx = np.arange(LANES)
    ang = 2.0 * np.pi * ((idx[:, None] * idx[None, :]) % LANES) / LANES
    c, s = np.cos(ang), sign * np.sin(ang)
    full = np.block([[c, s], [-s, c]])
    hi, lo = halves(full)
    return np.concatenate([hi, hi, lo], axis=0)


def doppler_table(pulses):
    part = pulses // RADIX
    m = np.arange(part)
    out = []
    for res in range(RADIX):
        ang = 2.0 * np.pi * ((m[None, :] * (RADIX * m[:, None] + res)) % pulses) / pulses
        c, s = np.cos(ang) / math.sqrt(pulses), -np.sin(ang) / math.sqrt(pulses)
        full = np.block([[c, -s], [s, c]])
        hi, lo = halves(full)
        out.append(np.concatenate([hi, hi, lo], axis=1))
    return np.stack(out)


def split(x, axis):
    hi = x.astype(jnp.bfloat16)
    lo = (x - hi.astype(jnp.float32)).astype(jnp.bfloat16)
    return jnp.concatenate([hi, lo, hi], axis=axis)


def fft_list(re, im, sign):
    n = len(re)
    if n == 1:
        return re, im
    er, ei = fft_list(re[0::2], im[0::2], sign)
    odd_r, odd_i = fft_list(re[1::2], im[1::2], sign)
    half = n // 2
    out_r, out_i = [None] * n, [None] * n
    for k in range(half):
        a, b = odd_r[k], odd_i[k]
        if k == 0:
            tr, ti = a, b
        elif 4 * k == n:
            tr, ti = (b, -a) if sign < 0 else (-b, a)
        elif 8 * k == n or 8 * k == 3 * n:
            h = math.sqrt(0.5)
            c = h if 8 * k == n else -h
            tr = c * a - (sign * h) * b
            ti = c * b + (sign * h) * a
        else:
            c = math.cos(2.0 * math.pi * k / n)
            s = sign * math.sin(2.0 * math.pi * k / n)
            tr = c * a - s * b
            ti = s * a + c * b
        out_r[k], out_i[k] = er[k] + tr, ei[k] + ti
        out_r[k + half], out_i[k + half] = er[k] - tr, ei[k] - ti
    return out_r, out_i


def range_rows(xs, c, r0, tw8, rep8, wf, wi, comp):
    n, per = comp.shape[1], comp.shape[2]
    cols = n * per
    rows = pl.ds(r0, SUB)
    re = [xs[0, c, rows, a * LANES:(a + 1) * LANES].astype(jnp.float32) for a in range(cols)]
    im = [xs[1, c, rows, a * LANES:(a + 1) * LANES].astype(jnp.float32) for a in range(cols)]
    re, im = fft_list(re, im, -1.0)
    mr, mi = jnp.concatenate(re, axis=0), jnp.concatenate(im, axis=0)
    tr, ti = tw8[0], tw8[1]
    m = jnp.concatenate([mr * tr - mi * ti, mr * ti + mi * tr], axis=1)
    f = jnp.dot(split(m, 1), wf[...], preferred_element_type=jnp.float32)
    fr, fi = f[:, :LANES], f[:, LANES:]
    tr, ti = rep8[0], rep8[1]
    m = jnp.concatenate([fr * tr - fi * ti, fr * ti + fi * tr], axis=1)
    f = jnp.dot(split(m, 1), wi[...], preferred_element_type=jnp.float32)
    fr, fi = f[:, :LANES], f[:, LANES:]
    tr, ti = tw8[0], tw8[1]
    mr, mi = fr * tr + fi * ti, fi * tr - fr * ti
    re = [mr[a * SUB:(a + 1) * SUB] for a in range(cols)]
    im = [mi[a * SUB:(a + 1) * SUB] for a in range(cols)]
    re, im = fft_list(re, im, 1.0)
    for j in range(n):
        for a in range(per):
            comp[c, j, a, 0, rows, :] = re[j * per + a]
            comp[c, j, a, 1, rows, :] = im[j * per + a]


def doppler_chunk(recv, c, g, table, pw, hi_ref, lo_ref):
    quarter = recv.shape[3] // RADIX
    a, b, cc, d = ([recv[c, g, ri, q * quarter:(q + 1) * quarter, :] for ri in range(2)] for q in range(RADIX))
    sr, si = a[0] + cc[0], a[1] + cc[1]
    dr, di = a[0] - cc[0], a[1] - cc[1]
    ur, ui = b[0] + d[0], b[1] + d[1]
    vr, vi = b[0] - d[0], b[1] - d[1]
    ys = [(sr + ur, si + ui), (dr + vi, di - vr), (sr - ur, si - ui), (dr - vi, di + vr)]
    for res in range(RADIX):
        y = jnp.concatenate(ys[res], axis=0)
        out = jnp.dot(table[res], split(y, 0), preferred_element_type=jnp.float32)
        re, im = out[:quarter], out[quarter:]
        p = re * re + im * im
        hi = p.astype(jnp.bfloat16)
        pw[c, g, res] = p
        hi_ref[c, g + 1, res] = hi
        lo_ref[c, g + 1, res] = (p - hi.astype(jnp.float32)).astype(jnp.bfloat16)


def cfar_chunk(c, g, first_gate, gates, thresh, window, pw, hi_ref, lo_ref, band, stage, out, acc):
    quarter = pw.shape[3]
    total = RADIX * quarter
    parts = [ref[c, g + k].reshape(total, LANES) for ref in (hi_ref, lo_ref) for k in range(3)]
    noise = jnp.dot(jnp.concatenate(parts, axis=1), band[c], preferred_element_type=jnp.float32)
    guard = window[c, 0]
    reach = guard + window[c, 1]
    gate = first_gate + g * LANES + lax.broadcasted_iota(jnp.int32, (SUB, LANES), 1)
    after = gates - 1 - gate
    cells = jnp.minimum(gate, reach) - jnp.minimum(gate, guard) + jnp.minimum(after, reach) - jnp.minimum(after, guard)
    cells = cells.astype(jnp.float32)[:1]
    inv = thresh[c, 1].astype(jnp.float32) / thresh[c, 0].astype(jnp.float32)
    ratio = pw[c, g].reshape(total, LANES) * cells / (noise + EPSILON)
    for res in range(RADIX):
        stage[pl.ds(res, quarter, stride=RADIX), :] = ratio[res * quarter:(res + 1) * quarter]
    out[c, :, pl.ds(pl.multiple_of(g * LANES, LANES), LANES)] = stage[...]
    soft = jnp.clip(ratio * inv - 1.0, 0.0, 1.0)
    acc[...] += jnp.sum(soft.reshape(total // SUB, SUB, LANES), axis=0)


def kernel(sizes, rep_hbm, thresh_hbm, window_hbm, x_hbm, tw_hbm, wf_hbm, wi_hbm, t_hbm, out, count,
           rep, thresh, window, tw, nat, xs, wf, wi, table, tw8, rep8, comp, recv, pw, hi_ref, lo_ref, band, stage, pack, halo, gather, acc,
           in_sem, tab_sem, row_send, row_recv, chunk_send, chunk_recv, halo_send, halo_recv, sum_sem):
    n, nx, ns, rows = sizes
    _, channels, part, gates = xs.shape
    chunks = comp.shape[2]
    quarter = pw.shape[3]
    pulses = RADIX * quarter
    own = gates // n
    blocks = part // rows
    last = channels - 1
    z, x, s = lax.axis_index("pulse"), lax.axis_index("chan"), lax.axis_index("sub")
    peers = n * nx * ns
    me = (z * nx + x) * ns + s
    h = n // 2
    half = z // h

    def peer(p):
        i = lax.rem(me + p, peers)
        return {"pulse": i // (nx * ns), "chan": lax.rem(i // ns, nx), "sub": lax.rem(i, ns)}

    barrier = pltpu.get_barrier_semaphore()

    def greet(p, carry):
        pl.semaphore_signal(barrier, 1, device_id=peer(p), device_id_type=MESH)
        return carry

    def load(b):
        c = b // blocks
        r = pl.ds(pl.multiple_of(lax.rem(b, blocks) * rows, rows), rows)
        return pltpu.make_async_copy(x_hbm.at[:, c, r, :], xs.at[:, c, r, :], in_sem.at[b])

    def start_load(b, carry):
        load(b).start()
        return carry

    tables = [pltpu.make_async_copy(a, b, tab_sem.at[i])
              for i, (a, b) in enumerate(((rep_hbm, rep), (tw_hbm, tw), (wf_hbm, wf), (wi_hbm, wi), (t_hbm, table),
                                         (thresh_hbm, thresh), (window_hbm, window)))]
    tables[0].start()
    load(0).start()
    for copy in tables[1:4]:
        copy.start()
    lax.fori_loop(1, peers, greet, 0)
    lax.fori_loop(1, channels * blocks, start_load, 0)
    for copy in tables[4:]:
        copy.start()
    cols = tw.shape[1]
    nat[...] = jnp.zeros_like(nat)
    tables[0].wait()
    for ri in range(2):
        for k in range(cols):
            nat[ri * cols + k:ri * cols + k + 1, :] = rep[ri:ri + 1, k * LANES:(k + 1) * LANES]
    turned = jnp.transpose(nat[...])
    row = lax.broadcasted_iota(jnp.int32, (LANES, LANES), 0)
    lane = lax.broadcasted_iota(jnp.int32, (LANES, LANES), 1)
    per = LANES // cols
    for ri in range(2):
        filt = jnp.zeros((cols, LANES), jnp.float32)
        for k in range(per):
            pick = jnp.where(jnp.logical_and(row >= ri * cols, lane == per * (row - ri * cols) + k), 1.0, 0.0)
            filt = filt + jnp.dot(turned[k * cols:(k + 1) * cols], pick, precision=lax.Precision.HIGHEST,
                                  preferred_element_type=jnp.float32)
        filt = filt * (INPUT_SCALE / gates)
        for k in range(cols):
            rep8[ri, k * SUB:(k + 1) * SUB, :] = jnp.broadcast_to(filt[k:k + 1, :], (SUB, LANES))
    tables[1].wait()
    for k in range(cols):
        for ri in range(2):
            tw8[ri, k * SUB:(k + 1) * SUB, :] = jnp.broadcast_to(tw[ri, k:k + 1, :], (SUB, LANES))

    def near(k):
        return half * h + lax.rem(lax.rem(z, h) + 1 + k, h)

    def cross(k):
        return (1 - half) * h + lax.rem(z + s + k, h)

    def row_copy(c, dest, b):
        r = pl.multiple_of(b * rows, rows)
        return pltpu.make_async_remote_copy(
            comp.at[c, dest, :, :, pl.ds(r, rows), :],
            recv.at[c, :, :, pl.ds(pl.multiple_of(z * part + r, rows), rows), :],
            row_send.at[c, dest], row_recv.at[c, z],
            device_id={"pulse": dest}, device_id_type=MESH)

    def row_all(c, dest, src):
        return pltpu.make_async_remote_copy(
            comp.at[c, dest], recv.at[c, :, :, pl.ds(pl.multiple_of(src * part, part), part), :],
            row_send.at[c, dest], row_recv.at[c, src],
            device_id={"pulse": dest}, device_id_type=MESH)

    def chunk_copy(dest, src, g):
        return pltpu.make_async_remote_copy(
            comp.at[last, dest, g], recv.at[last, g, :, pl.ds(pl.multiple_of(src * part, part), part), :],
            chunk_send.at[dest, g], chunk_recv.at[src, g],
            device_id={"pulse": dest}, device_id_type=MESH)

    outer = jnp.logical_and(n == 4, jnp.logical_or(z == 0, z == n - 1))

    def row_near(c, b):
        for k in range(h - 1):
            row_copy(c, near(k), b).start()

    def row_cross(c, b):
        for k in range(h):
            row_copy(c, cross(k), b).start()

    def step(b, carry):
        c = b // blocks
        r0 = lax.rem(b, blocks) * rows
        load(b).wait()

        @pl.when(b == 0)
        def _():
            tables[2].wait()
            tables[3].wait()

        for u in range(rows // SUB):
            range_rows(xs, c, pl.multiple_of(r0 + u * SUB, SUB), tw8, rep8, wf, wi, comp)

        @pl.when(b == 1)
        def _():
            pl.semaphore_wait(barrier, peers - 1)

        @pl.when(jnp.logical_and(b >= 1, b <= last * blocks))
        def _():
            pc, pb = (b - 1) // blocks, lax.rem(b - 1, blocks)

            @pl.when(outer)
            def _():
                row_near(pc, pb)

            @pl.when(jnp.logical_not(outer))
            def _():
                row_cross(pc, pb)

        return carry

    lax.fori_loop(0, channels * blocks, step, 0)

    def each(body, lo, hi):
        def run(i, carry):
            body(i)
            return carry
        lax.fori_loop(lo, hi, run, 0)

    def order(k):
        odd = lax.rem(k, 2)
        return odd * (chunks - 1) + (1 - 2 * odd) * (k // 2)

    def rest(t):
        c, b = t // blocks, lax.rem(t, blocks)

        @pl.when(outer)
        def _():
            row_cross(c, b)

        @pl.when(jnp.logical_not(outer))
        def _():
            row_near(c, b)

    def last_near(k):
        for q in range(h - 1):
            chunk_copy(near(q), z, order(k)).start()

    def far(q):
        return (1 - half) * (n - 1 - q) + half * q

    def last_cross(k):
        end = k // (chunks - 1) if chunks > 1 else 1
        for q in range(h):
            chunk_copy(end * far(q) + (1 - end) * cross(q), z, order(k)).start()

    ahead = min(AHEAD, chunks)
    each(last_near, 0, chunks)
    each(rest, 0, last * blocks)
    each(last_cross, 0, ahead)

    def keep(t):
        c, g = t // chunks, lax.rem(t, chunks)
        for ri in range(2):
            recv[c, g, ri, pl.ds(pl.multiple_of(z * part, part), part), :] = comp[c, z, g, ri]

    each(keep, 0, channels * chunks)
    for copy in tables[4:]:
        copy.wait()
    q = lax.broadcasted_iota(jnp.int32, (3 * LANES, LANES), 0)
    j = lax.broadcasted_iota(jnp.int32, (3 * LANES, LANES), 1)
    dist = jnp.abs(q - LANES - j)
    for c in range(channels):
        guard = window[c, 0]
        reach = guard + window[c, 1]
        inside = jnp.where(dist > guard, 1.0, 0.0) * jnp.where(dist <= reach, 1.0, 0.0)
        inside = inside.astype(jnp.bfloat16)
        band[c] = jnp.concatenate([inside, inside], axis=0)
        blank = jnp.zeros((RADIX, quarter, LANES), jnp.bfloat16)
        for ref in (hi_ref, lo_ref):
            ref[c, 0] = blank
            ref[c, chunks + 1] = blank
    acc[...] = jnp.zeros_like(acc)

    def dop(c, g):
        doppler_chunk(recv, c, g, table, pw, hi_ref, lo_ref)

    def cfar(c, g):
        cfar_chunk(c, g, z * own, gates, thresh, window, pw, hi_ref, lo_ref, band, stage, out, acc)

    def pack_left(c):
        pack[c, 0] = jnp.concatenate([pw[c, 0, res][:, :MARGIN] for res in range(RADIX)], axis=1)

    def pack_right(c):
        pack[c, 1] = jnp.concatenate([pw[c, chunks - 1, res][:, LANES - MARGIN:] for res in range(RADIX)], axis=1)

    def halo_copy(c, side, dest):
        return pltpu.make_async_remote_copy(
            pack.at[c, side], halo.at[c, 1 - side], halo_send.at[c, side], halo_recv.at[c, 1 - side],
            device_id={"pulse": dest}, device_id_type=MESH)

    def send_halo(c):
        @pl.when(z > 0)
        def _():
            halo_copy(c, 0, z - 1).start()

        @pl.when(z < n - 1)
        def _():
            halo_copy(c, 1, z + 1).start()

    def unpack(c, side):
        for res in range(RADIX):
            turn = (LANES - MARGIN - MARGIN * res if side == 0 else LANES - MARGIN * res) % LANES
            p = halo[c, side]
            if turn:
                p = pltpu.roll(p, turn, 1)
            hi = p.astype(jnp.bfloat16)
            at = 0 if side == 0 else chunks + 1
            hi_ref[c, at, res] = hi
            lo_ref[c, at, res] = (p - hi.astype(jnp.float32)).astype(jnp.bfloat16)

    def take_halo(c):
        @pl.when(z > 0)
        def _():
            halo_copy(c, 1, z).wait_recv()
            unpack(c, 0)

        @pl.when(z < n - 1)
        def _():
            halo_copy(c, 0, z).wait_recv()
            unpack(c, 1)

    for c in range(last):
        for o in range(1, n):
            row_all(c, z, lax.rem(z + o, n)).wait_recv()
        each(functools.partial(dop, c), 0, chunks)
        pack_left(c)
        pack_right(c)
        if chunks > 2:
            cfar(c, 1)
        send_halo(c)
        each(functools.partial(cfar, c), 2, chunks - 1)

    def arrive(k):
        for o in range(1, n):
            chunk_copy(z, lax.rem(z + o, n), order(k)).wait_recv()

    head = chunks - 1 if chunks >= 4 else chunks

    def last_step(k):
        @pl.when(k + ahead < chunks)
        def _():
            last_cross(k + ahead)

        arrive(k)
        dop(last, order(k))

        @pl.when(k == 0)
        def _():
            pack_left(last)

        @pl.when(k == min(1, chunks - 1))
        def _():
            pack_right(last)

        if chunks >= 4:
            @pl.when(k == 2)
            def _():
                send_halo(last)

            @pl.when(k >= 4)
            def _():
                cfar(last, order(k - 2))

    each(last_step, 0, head)
    if chunks < 4:
        send_halo(last)
        each(functools.partial(cfar, last), 1, chunks - 1)
    for c in range(channels):
        take_halo(c)
    edges = min(2, chunks)

    def edge(t):
        cfar(t // edges, lax.rem(t, edges) * (chunks - 1))

    each(edge, 0, channels * edges)
    if chunks >= 4:
        arrive(chunks - 1)
        dop(last, order(jnp.int32(chunks - 1)))
        each(lambda k: cfar(last, order(k)), chunks - 3, chunks)

    gather[me] = jnp.sum(acc[...], axis=0, keepdims=True)
    for c in range(last):
        for o in range(1, n):
            row_all(c, lax.rem(z + o, n), z).wait_send()

    def sent(g):
        for o in range(1, n):
            chunk_copy(lax.rem(z + o, n), z, g).wait_send()

    each(sent, 0, chunks)
    for c in range(channels):
        @pl.when(z > 0)
        def _():
            halo_copy(c, 0, z - 1).wait_send()

        @pl.when(z < n - 1)
        def _():
            halo_copy(c, 1, z + 1).wait_send()

    def tell(p):
        pltpu.make_async_remote_copy(
            gather.at[me], gather.at[me], sum_sem.at[0], sum_sem.at[1],
            device_id=peer(p), device_id_type=MESH).start()

    each(tell, 1, peers)
    every = pltpu.make_async_remote_copy(
        gather.at[pl.ds(0, peers - 1)], gather.at[pl.ds(0, peers - 1)], sum_sem.at[0], sum_sem.at[1],
        device_id=peer(1), device_id_type=MESH)
    every.wait()
    total = jnp.sum(gather[...], axis=0)
    count[0] = jnp.sum(total) * (1024.0 / (pulses * gates))


def local(samples, replica, window, thresh):
    _, channels, part, gates = samples.shape
    n, nx, ns = (lax.axis_size(a) for a in ("pulse", "chan", "sub"))
    cols = gates // LANES
    pulses = part * n
    own = gates // n
    chunks = own // LANES
    quarter = pulses // RADIX
    rows = min(ROWS, part)
    k1 = np.arange(cols)[:, None]
    b = np.arange(LANES)[None, :]
    ang = 2.0 * np.pi * ((k1 * b) % gates) / gates
    tw = np.stack([np.cos(ang), -np.sin(ang)]).astype(np.float32)
    wf, wi = lane_table(-1.0), lane_table(1.0)
    table = doppler_table(pulses)
    peers = n * nx * ns
    f32, bf16 = jnp.float32, jnp.bfloat16
    smem, vmem, hbm = (pl.BlockSpec(memory_space=m) for m in (pltpu.SMEM, pltpu.VMEM, pltpu.HBM))
    dma = pltpu.SemaphoreType.DMA
    return pl.pallas_call(
        functools.partial(kernel, (n, nx, ns, rows)),
        in_specs=[hbm] * 8,
        out_specs=[vmem, smem],
        out_shape=[pltpu.VMEM((channels, pulses, own), f32), jax.ShapeDtypeStruct((1,), f32)],
        scratch_shapes=[
            pltpu.VMEM(replica.shape, f32),
            pltpu.SMEM(thresh.shape, jnp.int32),
            pltpu.SMEM(window.shape, jnp.int32),
            pltpu.VMEM(tw.shape, f32),
            pltpu.VMEM((LANES, LANES), f32),
            pltpu.VMEM((2, channels, part, gates), jnp.int32),
            pltpu.VMEM(wf.shape, bf16),
            pltpu.VMEM(wi.shape, bf16),
            pltpu.VMEM(table.shape, bf16),
            pltpu.VMEM((2, cols * SUB, LANES), f32),
            pltpu.VMEM((2, cols * SUB, LANES), f32),
            pltpu.VMEM((channels, n, chunks, 2, part, LANES), f32),
            pltpu.VMEM((channels, chunks, 2, pulses, LANES), f32),
            pltpu.VMEM((channels, chunks, RADIX, quarter, LANES), f32),
            pltpu.VMEM((channels, chunks + 2, RADIX, quarter, LANES), bf16),
            pltpu.VMEM((channels, chunks + 2, RADIX, quarter, LANES), bf16),
            pltpu.VMEM((channels, 6 * LANES, LANES), bf16),
            pltpu.VMEM((pulses, LANES), f32),
            pltpu.VMEM((channels, 2, quarter, LANES), f32),
            pltpu.VMEM((channels, 2, quarter, LANES), f32),
            pltpu.VMEM((peers, 1, LANES), f32),
            pltpu.VMEM((SUB, LANES), f32),
            dma((channels * (part // rows),)),
            dma((7,)),
            dma((channels, n)),
            dma((channels, n)),
            dma((n, chunks)),
            dma((n, chunks)),
            dma((channels, 2)),
            dma((channels, 2)),
            dma((2,)),
        ],
        compiler_params=pltpu.CompilerParams(
            collective_id=0, has_side_effects=True, vmem_limit_bytes=48 << 20),
        cost_estimate=pl.CostEstimate(flops=int(2e10), bytes_accessed=32 << 20, transcendentals=0),
    )(*(pltpu.with_memory_space_constraint(jnp.asarray(a), pltpu.HBM)
        for a in (replica, thresh, window, samples, tw, wf, wi, table)))


def solution(mesh):
    in_specs = (
        P(None, ("grp", "chan", "sub"), "pulse", None),
        P(),
        P(("grp", "chan", "sub"), None),
        P(("grp", "chan", "sub"), None),
    )
    out_specs = (P(("grp", "chan", "sub"), None, "pulse"), P("grp"))
    return jax.shard_map(lambda *a: tuple(local(*a)), mesh=mesh, in_specs=in_specs, out_specs=out_specs, check_vma=False)
```

```python
import functools
import math

import jax
import jax.numpy as jnp
import numpy as np
from jax import lax
from jax.experimental import pallas as pl
from jax.experimental.pallas import tpu as pltpu
from jax.sharding import PartitionSpec as P

GUARD_MAX = 4
TRAIN_MAX = 28
MARGIN = GUARD_MAX + TRAIN_MAX
EPSILON = 1e-06
INPUT_SCALE = 1.0 / 2048.0
LANES = 128
SUB = 8
RADIX = 4


def halves(table):
    hi = np.asarray(table, np.float32).astype(jnp.bfloat16)
    lo = (np.asarray(table, np.float64) - hi.astype(np.float64)).astype(jnp.bfloat16)
    return hi, lo


MESH = pl.DeviceIdType.MESH
ROWS = 8
AHEAD = 3


def lane_table(sign):
    idx = np.arange(LANES)
    ang = 2.0 * np.pi * ((idx[:, None] * idx[None, :]) % LANES) / LANES
    c, s = np.cos(ang), sign * np.sin(ang)
    full = np.block([[c, s], [-s, c]])
    hi, lo = halves(full)
    return np.concatenate([hi, hi, lo], axis=0)


def doppler_table(pulses):
    part = pulses // RADIX
    m = np.arange(part)
    out = []
    for res in range(RADIX):
        ang = 2.0 * np.pi * ((m[None, :] * (RADIX * m[:, None] + res)) % pulses) / pulses
        c, s = np.cos(ang) / math.sqrt(pulses), -np.sin(ang) / math.sqrt(pulses)
        full = np.block([[c, -s], [s, c]])
        hi, lo = halves(full)
        out.append(np.concatenate([hi, hi, lo], axis=1))
    return np.stack(out)


def split(x, axis):
    hi = x.astype(jnp.bfloat16)
    lo = (x - hi.astype(jnp.float32)).astype(jnp.bfloat16)
    return jnp.concatenate([hi, lo, hi], axis=axis)


def fft_list(re, im, sign):
    n = len(re)
    if n == 1:
        return re, im
    er, ei = fft_list(re[0::2], im[0::2], sign)
    odd_r, odd_i = fft_list(re[1::2], im[1::2], sign)
    half = n // 2
    out_r, out_i = [None] * n, [None] * n
    for k in range(half):
        a, b = odd_r[k], odd_i[k]
        if k == 0:
            tr, ti = a, b
        elif 4 * k == n:
            tr, ti = (b, -a) if sign < 0 else (-b, a)
        elif 8 * k == n or 8 * k == 3 * n:
            h = math.sqrt(0.5)
            c = h if 8 * k == n else -h
            tr = c * a - (sign * h) * b
            ti = c * b + (sign * h) * a
        else:
            c = math.cos(2.0 * math.pi * k / n)
            s = sign * math.sin(2.0 * math.pi * k / n)
            tr = c * a - s * b
            ti = s * a + c * b
        out_r[k], out_i[k] = er[k] + tr, ei[k] + ti
        out_r[k + half], out_i[k + half] = er[k] - tr, ei[k] - ti
    return out_r, out_i


def range_rows(xs, c, r0, tw8, rep8, wf, wi, comp):
    n, per = comp.shape[1], comp.shape[2]
    cols = n * per
    rows = pl.ds(r0, SUB)
    re = [xs[0, c, rows, a * LANES:(a + 1) * LANES].astype(jnp.float32) for a in range(cols)]
    im = [xs[1, c, rows, a * LANES:(a + 1) * LANES].astype(jnp.float32) for a in range(cols)]
    re, im = fft_list(re, im, -1.0)
    mr, mi = jnp.concatenate(re, axis=0), jnp.concatenate(im, axis=0)
    tr, ti = tw8[0], tw8[1]
    m = jnp.concatenate([mr * tr - mi * ti, mr * ti + mi * tr], axis=1)
    f = jnp.dot(split(m, 1), wf[...], preferred_element_type=jnp.float32)
    fr, fi = f[:, :LANES], f[:, LANES:]
    tr, ti = rep8[0], rep8[1]
    m = jnp.concatenate([fr * tr - fi * ti, fr * ti + fi * tr], axis=1)
    f = jnp.dot(split(m, 1), wi[...], preferred_element_type=jnp.float32)
    fr, fi = f[:, :LANES], f[:, LANES:]
    tr, ti = tw8[0], tw8[1]
    mr, mi = fr * tr + fi * ti, fi * tr - fr * ti
    re = [mr[a * SUB:(a + 1) * SUB] for a in range(cols)]
    im = [mi[a * SUB:(a + 1) * SUB] for a in range(cols)]
    re, im = fft_list(re, im, 1.0)
    for j in range(n):
        for a in range(per):
            comp[c, j, a, 0, rows, :] = re[j * per + a]
            comp[c, j, a, 1, rows, :] = im[j * per + a]


def doppler_chunk(recv, c, g, table, pw, hi_ref, lo_ref):
    quarter = recv.shape[3] // RADIX
    a, b, cc, d = ([recv[c, g, ri, q * quarter:(q + 1) * quarter, :] for ri in range(2)] for q in range(RADIX))
    sr, si = a[0] + cc[0], a[1] + cc[1]
    dr, di = a[0] - cc[0], a[1] - cc[1]
    ur, ui = b[0] + d[0], b[1] + d[1]
    vr, vi = b[0] - d[0], b[1] - d[1]
    ys = [(sr + ur, si + ui), (dr + vi, di - vr), (sr - ur, si - ui), (dr - vi, di + vr)]
    for res in range(RADIX):
        y = jnp.concatenate(ys[res], axis=0)
        out = jnp.dot(table[res], split(y, 0), preferred_element_type=jnp.float32)
        re, im = out[:quarter], out[quarter:]
        p = re * re + im * im
        hi = p.astype(jnp.bfloat16)
        pw[c, g, res] = p
        hi_ref[c, g + 1, res] = hi
        lo_ref[c, g + 1, res] = (p - hi.astype(jnp.float32)).astype(jnp.bfloat16)


def cfar_chunk(c, g, first_gate, gates, thresh, window, pw, hi_ref, lo_ref, band, stage, out, acc):
    quarter = pw.shape[3]
    total = RADIX * quarter
    parts = [ref[c, g + k].reshape(total, LANES) for ref in (hi_ref, lo_ref) for k in range(3)]
    noise = jnp.dot(jnp.concatenate(parts, axis=1), band[c], preferred_element_type=jnp.float32)
    guard = window[c, 0]
    reach = guard + window[c, 1]
    gate = first_gate + g * LANES + lax.broadcasted_iota(jnp.int32, (SUB, LANES), 1)
    after = gates - 1 - gate
    cells = jnp.minimum(gate, reach) - jnp.minimum(gate, guard) + jnp.minimum(after, reach) - jnp.minimum(after, guard)
    cells = cells.astype(jnp.float32)[:1]
    inv = thresh[c, 1].astype(jnp.float32) / thresh[c, 0].astype(jnp.float32)
    ratio = pw[c, g].reshape(total, LANES) * cells / (noise + EPSILON)
    for res in range(RADIX):
        stage[pl.ds(res, quarter, stride=RADIX), :] = ratio[res * quarter:(res + 1) * quarter]
    out[c, :, pl.ds(pl.multiple_of(g * LANES, LANES), LANES)] = stage[...]
    soft = jnp.clip(ratio * inv - 1.0, 0.0, 1.0)
    acc[...] += jnp.sum(soft.reshape(total // SUB, SUB, LANES), axis=0)


def kernel(sizes, rep_hbm, thresh_hbm, window_hbm, x_hbm, tw_hbm, wf_hbm, wi_hbm, t_hbm, out, count,
           rep, thresh, window, tw, nat, xs, wf, wi, table, tw8, rep8, comp, recv, pw, hi_ref, lo_ref, band, stage, pack, halo, gather, acc,
           in_sem, tab_sem, row_send, row_recv, chunk_send, chunk_recv, halo_send, halo_recv, sum_sem):
    n, nx, ns, rows = sizes
    _, channels, part, gates = xs.shape
    chunks = comp.shape[2]
    quarter = pw.shape[3]
    pulses = RADIX * quarter
    own = gates // n
    blocks = part // rows
    last = channels - 1
    z, x, s = lax.axis_index("pulse"), lax.axis_index("chan"), lax.axis_index("sub")
    peers = n * nx * ns
    me = (z * nx + x) * ns + s
    h = n // 2
    half = z // h

    def others(act):
        def along(o, carry):
            for ox in range(nx):
                for os in range(ns):
                    act({"pulse": lax.rem(z + o, n), "chan": lax.rem(x + ox, nx), "sub": lax.rem(s + os, ns)})
            return carry
        lax.fori_loop(1, n, along, 0, unroll=n <= 4)
        for ox in range(nx):
            for os in range(ns):
                if ox or os:
                    act({"pulse": z, "chan": lax.rem(x + ox, nx), "sub": lax.rem(s + os, ns)})

    barrier = pltpu.get_barrier_semaphore()

    others(lambda who: pl.semaphore_signal(barrier, 1, device_id=who, device_id_type=MESH))

    def load(b):
        c = b // blocks
        r = pl.ds(pl.multiple_of(lax.rem(b, blocks) * rows, rows), rows)
        return pltpu.make_async_copy(x_hbm.at[:, c, r, :], xs.at[:, c, r, :], in_sem.at[b])

    tables = [pltpu.make_async_copy(a, b, tab_sem.at[i])
              for i, (a, b) in enumerate(((rep_hbm, rep), (tw_hbm, tw), (wf_hbm, wf), (wi_hbm, wi), (t_hbm, table),
                                         (thresh_hbm, thresh), (window_hbm, window)))]
    tables[0].start()
    load(0).start()
    for copy in tables[1:4]:
        copy.start()
    for b in range(1, min(2, channels * blocks)):
        load(b).start()
    cols = tw.shape[1]
    nat[...] = jnp.zeros_like(nat)
    tables[0].wait()
    for ri in range(2):
        for k in range(cols):
            nat[ri * cols + k:ri * cols + k + 1, :] = rep[ri:ri + 1, k * LANES:(k + 1) * LANES]
    turned = jnp.transpose(nat[...])
    row = lax.broadcasted_iota(jnp.int32, (LANES, LANES), 0)
    lane = lax.broadcasted_iota(jnp.int32, (LANES, LANES), 1)
    per = LANES // cols
    for ri in range(2):
        filt = jnp.zeros((cols, LANES), jnp.float32)
        for k in range(per):
            pick = jnp.where(jnp.logical_and(row >= ri * cols, lane == per * (row - ri * cols) + k), 1.0, 0.0)
            filt = filt + jnp.dot(turned[k * cols:(k + 1) * cols], pick, precision=lax.Precision.HIGHEST,
                                  preferred_element_type=jnp.float32)
        filt = filt * (INPUT_SCALE / gates)
        for k in range(cols):
            rep8[ri, k * SUB:(k + 1) * SUB, :] = jnp.broadcast_to(filt[k:k + 1, :], (SUB, LANES))
    tables[1].wait()
    for k in range(cols):
        for ri in range(2):
            tw8[ri, k * SUB:(k + 1) * SUB, :] = jnp.broadcast_to(tw[ri, k:k + 1, :], (SUB, LANES))

    def near(k):
        return half * h + lax.rem(lax.rem(z, h) + 1 + k, h)

    def cross(k):
        return (1 - half) * h + lax.rem(z + s + k, h)

    def row_copy(c, dest, b):
        r = pl.multiple_of(b * rows, rows)
        return pltpu.make_async_remote_copy(
            comp.at[c, dest, :, :, pl.ds(r, rows), :],
            recv.at[c, :, :, pl.ds(pl.multiple_of(z * part + r, rows), rows), :],
            row_send.at[c, dest], row_recv.at[c, z],
            device_id={"pulse": dest}, device_id_type=MESH)

    def row_all(c, dest, src):
        return pltpu.make_async_remote_copy(
            comp.at[c, dest], recv.at[c, :, :, pl.ds(pl.multiple_of(src * part, part), part), :],
            row_send.at[c, dest], row_recv.at[c, src],
            device_id={"pulse": dest}, device_id_type=MESH)

    def chunk_copy(dest, src, g):
        return pltpu.make_async_remote_copy(
            comp.at[last, dest, g], recv.at[last, g, :, pl.ds(pl.multiple_of(src * part, part), part), :],
            chunk_send.at[dest, g], chunk_recv.at[src, g],
            device_id={"pulse": dest}, device_id_type=MESH)

    outer = jnp.logical_and(n == 4, jnp.logical_or(z == 0, z == n - 1))

    def row_near(c, b):
        for k in range(h - 1):
            row_copy(c, near(k), b).start()

    def row_cross(c, b):
        for k in range(h):
            row_copy(c, cross(k), b).start()

    def step(b, carry):
        c = b // blocks
        r0 = lax.rem(b, blocks) * rows
        load(b).wait()

        @pl.when(b + 2 < channels * blocks)
        def _():
            load(b + 2).start()

        @pl.when(b == 0)
        def _():
            tables[2].wait()
            tables[3].wait()
            for copy in tables[4:]:
                copy.start()

        for u in range(rows // SUB):
            range_rows(xs, c, pl.multiple_of(r0 + u * SUB, SUB), tw8, rep8, wf, wi, comp)

        @pl.when(b == 1)
        def _():
            pl.semaphore_wait(barrier, peers - 1)

        @pl.when(jnp.logical_and(b >= 1, b <= last * blocks))
        def _():
            pc, pb = (b - 1) // blocks, lax.rem(b - 1, blocks)

            @pl.when(outer)
            def _():
                row_near(pc, pb)

            @pl.when(jnp.logical_not(outer))
            def _():
                row_cross(pc, pb)

        return carry

    lax.fori_loop(0, channels * blocks, step, 0)

    def each(body, lo, hi):
        def run(i, carry):
            body(i)
            return carry
        lax.fori_loop(lo, hi, run, 0)

    def order(k):
        odd = lax.rem(k, 2)
        return odd * (chunks - 1) + (1 - 2 * odd) * (k // 2)

    def rest(t):
        c, b = t // blocks, lax.rem(t, blocks)

        @pl.when(outer)
        def _():
            row_cross(c, b)

        @pl.when(jnp.logical_not(outer))
        def _():
            row_near(c, b)

    def last_near(k):
        for q in range(h - 1):
            chunk_copy(near(q), z, order(k)).start()

    def far(q):
        return (1 - half) * (n - 1 - q) + half * q

    def last_cross(k):
        end = k // (chunks - 1) if chunks > 1 else 1
        for q in range(h):
            chunk_copy(end * far(q) + (1 - end) * cross(q), z, order(k)).start()

    ahead = min(AHEAD, chunks)
    each(last_near, 0, chunks)
    each(rest, 0, last * blocks)
    each(last_cross, 0, ahead)

    def keep(t):
        c, g = t // chunks, lax.rem(t, chunks)
        for ri in range(2):
            recv[c, g, ri, pl.ds(pl.multiple_of(z * part, part), part), :] = comp[c, z, g, ri]

    each(keep, 0, channels * chunks)
    for copy in tables[4:]:
        copy.wait()
    q = lax.broadcasted_iota(jnp.int32, (3 * LANES, LANES), 0)
    j = lax.broadcasted_iota(jnp.int32, (3 * LANES, LANES), 1)
    dist = jnp.abs(q - LANES - j)
    for c in range(channels):
        guard = window[c, 0]
        reach = guard + window[c, 1]
        inside = jnp.where(dist > guard, 1.0, 0.0) * jnp.where(dist <= reach, 1.0, 0.0)
        inside = inside.astype(jnp.bfloat16)
        band[c] = jnp.concatenate([inside, inside], axis=0)
        blank = jnp.zeros((RADIX, quarter, LANES), jnp.bfloat16)
        for ref in (hi_ref, lo_ref):
            ref[c, 0] = blank
            ref[c, chunks + 1] = blank
    acc[...] = jnp.zeros_like(acc)

    def dop(c, g):
        doppler_chunk(recv, c, g, table, pw, hi_ref, lo_ref)

    def cfar(c, g):
        cfar_chunk(c, g, z * own, gates, thresh, window, pw, hi_ref, lo_ref, band, stage, out, acc)

    def pack_left(c):
        pack[c, 0] = jnp.concatenate([pw[c, 0, res][:, :MARGIN] for res in range(RADIX)], axis=1)

    def pack_right(c):
        pack[c, 1] = jnp.concatenate([pw[c, chunks - 1, res][:, LANES - MARGIN:] for res in range(RADIX)], axis=1)

    def halo_copy(c, side, dest):
        return pltpu.make_async_remote_copy(
            pack.at[c, side], halo.at[c, 1 - side], halo_send.at[c, side], halo_recv.at[c, 1 - side],
            device_id={"pulse": dest}, device_id_type=MESH)

    def send_halo(c):
        @pl.when(z > 0)
        def _():
            halo_copy(c, 0, z - 1).start()

        @pl.when(z < n - 1)
        def _():
            halo_copy(c, 1, z + 1).start()

    def unpack(c, side):
        for res in range(RADIX):
            turn = (LANES - MARGIN - MARGIN * res if side == 0 else LANES - MARGIN * res) % LANES
            p = halo[c, side]
            if turn:
                p = pltpu.roll(p, turn, 1)
            hi = p.astype(jnp.bfloat16)
            at = 0 if side == 0 else chunks + 1
            hi_ref[c, at, res] = hi
            lo_ref[c, at, res] = (p - hi.astype(jnp.float32)).astype(jnp.bfloat16)

    def take_halo(c):
        @pl.when(z > 0)
        def _():
            halo_copy(c, 1, z).wait_recv()
            unpack(c, 0)

        @pl.when(z < n - 1)
        def _():
            halo_copy(c, 0, z).wait_recv()
            unpack(c, 1)

    for c in range(last):
        for o in range(1, n):
            row_all(c, z, lax.rem(z + o, n)).wait_recv()
        each(functools.partial(dop, c), 0, chunks)
        pack_left(c)
        pack_right(c)
        if chunks > 2:
            cfar(c, 1)
        send_halo(c)
        each(functools.partial(cfar, c), 2, chunks - 1)

    def arrive(k):
        for o in range(1, n):
            chunk_copy(z, lax.rem(z + o, n), order(k)).wait_recv()

    head = chunks - 1 if chunks >= 4 else chunks

    def last_step(k):
        @pl.when(k + ahead < chunks)
        def _():
            last_cross(k + ahead)

        arrive(k)
        dop(last, order(k))

        @pl.when(k == 0)
        def _():
            pack_left(last)

        @pl.when(k == min(1, chunks - 1))
        def _():
            pack_right(last)

        if chunks >= 4:
            @pl.when(k == 2)
            def _():
                send_halo(last)

            @pl.when(k >= 4)
            def _():
                cfar(last, order(k - 2))

    each(last_step, 0, head)
    if chunks < 4:
        send_halo(last)
        each(functools.partial(cfar, last), 1, chunks - 1)
    for c in range(channels):
        take_halo(c)
    edges = min(2, chunks)

    def edge(t):
        cfar(t // edges, lax.rem(t, edges) * (chunks - 1))

    each(edge, 0, channels * edges)
    if chunks >= 4:
        arrive(chunks - 1)
        dop(last, order(jnp.int32(chunks - 1)))
        for k in range(chunks - 3, chunks):
            cfar(last, (k % 2) * (chunks - 1) + (1 - 2 * (k % 2)) * (k // 2))

    gather[me] = jnp.sum(acc[...], axis=0, keepdims=True)
    for c in range(channels):
        @pl.when(z > 0)
        def _():
            halo_copy(c, 0, z - 1).wait_send()

        @pl.when(z < n - 1)
        def _():
            halo_copy(c, 1, z + 1).wait_send()

    def tell(who):
        pltpu.make_async_remote_copy(
            gather.at[me], gather.at[me], sum_sem.at[0], sum_sem.at[1],
            device_id=who, device_id_type=MESH).start()

    others(tell)
    for c in range(last):
        for o in range(1, n):
            row_all(c, lax.rem(z + o, n), z).wait_send()

    def sent(g):
        for o in range(1, n):
            chunk_copy(lax.rem(z + o, n), z, g).wait_send()

    each(sent, 0, chunks)
    every = pltpu.make_async_remote_copy(
        gather.at[pl.ds(0, peers - 1)], gather.at[pl.ds(0, peers - 1)], sum_sem.at[0], sum_sem.at[1],
        device_id={"pulse": lax.rem(z + 1, n)}, device_id_type=MESH)
    every.wait_recv()
    total = jnp.sum(gather[...], axis=0)
    total = jnp.sum(total, axis=1, keepdims=True) * (1024.0 / (pulses * gates))
    count[...] = jnp.broadcast_to(total, count.shape)
    every.wait_send()


def deliver_kernel(ratio, count, ratio_out, count_out, one, sem):
    channels, pulses, _ = ratio.shape
    step = pulses // 8
    one[0] = count[0, 0]
    copies = [pltpu.make_async_copy(one, count_out, sem.at[0])]
    for i in range(8 * channels):
        c, r = i // 8, pl.ds(i % 8 * step, step)
        copies.append(pltpu.make_async_copy(ratio.at[c, r], ratio_out.at[c, r], sem.at[i + 1]))
    for copy in copies:
        copy.start()
    for copy in copies:
        copy.wait()


def deliver(ratio, count):
    return pl.pallas_call(
        deliver_kernel,
        in_specs=[pl.BlockSpec(memory_space=pltpu.VMEM)] * 2,
        out_specs=[pl.BlockSpec(memory_space=pltpu.HBM)] * 2,
        out_shape=[jax.ShapeDtypeStruct(ratio.shape, jnp.float32), jax.ShapeDtypeStruct((1,), jnp.float32)],
        scratch_shapes=[pltpu.SMEM((1,), jnp.float32), pltpu.SemaphoreType.DMA((8 * ratio.shape[0] + 1,))],
        compiler_params=pltpu.CompilerParams(vmem_limit_bytes=1 << 20),
    )(*(pltpu.with_memory_space_constraint(a, pltpu.VMEM) for a in (ratio, count)))


def local(samples, replica, window, thresh):
    _, channels, part, gates = samples.shape
    n, nx, ns = (lax.axis_size(a) for a in ("pulse", "chan", "sub"))
    cols = gates // LANES
    pulses = part * n
    own = gates // n
    chunks = own // LANES
    quarter = pulses // RADIX
    rows = min(ROWS, part)
    k1 = np.arange(cols)[:, None]
    b = np.arange(LANES)[None, :]
    ang = 2.0 * np.pi * ((k1 * b) % gates) / gates
    tw = np.stack([np.cos(ang), -np.sin(ang)]).astype(np.float32)
    wf, wi = lane_table(-1.0), lane_table(1.0)
    table = doppler_table(pulses)
    peers = n * nx * ns
    f32, bf16 = jnp.float32, jnp.bfloat16
    vmem, hbm = (pl.BlockSpec(memory_space=m) for m in (pltpu.VMEM, pltpu.HBM))
    dma = pltpu.SemaphoreType.DMA
    return deliver(*pl.pallas_call(
        functools.partial(kernel, (n, nx, ns, rows)),
        in_specs=[hbm] * 8,
        out_specs=[vmem, vmem],
        out_shape=[pltpu.VMEM((channels, pulses, own), f32), pltpu.VMEM((1, LANES), f32)],
        scratch_shapes=[
            pltpu.VMEM(replica.shape, f32),
            pltpu.SMEM(thresh.shape, jnp.int32),
            pltpu.SMEM(window.shape, jnp.int32),
            pltpu.VMEM(tw.shape, f32),
            pltpu.VMEM((LANES, LANES), f32),
            pltpu.VMEM((2, channels, part, gates), jnp.int32),
            pltpu.VMEM(wf.shape, bf16),
            pltpu.VMEM(wi.shape, bf16),
            pltpu.VMEM(table.shape, bf16),
            pltpu.VMEM((2, cols * SUB, LANES), f32),
            pltpu.VMEM((2, cols * SUB, LANES), f32),
            pltpu.VMEM((channels, n, chunks, 2, part, LANES), f32),
            pltpu.VMEM((channels, chunks, 2, pulses, LANES), f32),
            pltpu.VMEM((channels, chunks, RADIX, quarter, LANES), f32),
            pltpu.VMEM((channels, chunks + 2, RADIX, quarter, LANES), bf16),
            pltpu.VMEM((channels, chunks + 2, RADIX, quarter, LANES), bf16),
            pltpu.VMEM((channels, 6 * LANES, LANES), bf16),
            pltpu.VMEM((pulses, LANES), f32),
            pltpu.VMEM((channels, 2, quarter, LANES), f32),
            pltpu.VMEM((channels, 2, quarter, LANES), f32),
            pltpu.VMEM((peers, 1, LANES), f32),
            pltpu.VMEM((SUB, LANES), f32),
            dma((channels * (part // rows),)),
            dma((7,)),
            dma((channels, n)),
            dma((channels, n)),
            dma((n, chunks)),
            dma((n, chunks)),
            dma((channels, 2)),
            dma((channels, 2)),
            dma((2,)),
        ],
        compiler_params=pltpu.CompilerParams(
            collective_id=0, has_side_effects=True, vmem_limit_bytes=48 << 20),
        cost_estimate=pl.CostEstimate(flops=int(2e10), bytes_accessed=32 << 20, transcendentals=0),
    )(*(pltpu.with_memory_space_constraint(jnp.asarray(a), pltpu.HBM)
        for a in (replica, thresh, window, samples, tw, wf, wi, table))))


def solution(mesh):
    in_specs = (
        P(None, ("grp", "chan", "sub"), "pulse", None),
        P(),
        P(("grp", "chan", "sub"), None),
        P(("grp", "chan", "sub"), None),
    )
    out_specs = (P(("grp", "chan", "sub"), None, "pulse"), P("grp"))
    return jax.shard_map(lambda *a: tuple(local(*a)), mesh=mesh, in_specs=in_specs, out_specs=out_specs, check_vma=False)
```

```python
import functools
import math

import jax
import jax.numpy as jnp
import numpy as np
from jax import lax
from jax.experimental import pallas as pl
from jax.experimental.pallas import tpu as pltpu
from jax.sharding import PartitionSpec as P

GUARD_MAX = 4
TRAIN_MAX = 28
MARGIN = GUARD_MAX + TRAIN_MAX
EPSILON = 1e-06
INPUT_SCALE = 1.0 / 2048.0
LANES = 128
SUB = 8
RADIX = 4


def halves(table):
    hi = np.asarray(table, np.float32).astype(jnp.bfloat16)
    lo = (np.asarray(table, np.float64) - hi.astype(np.float64)).astype(jnp.bfloat16)
    return hi, lo


MESH = pl.DeviceIdType.MESH
ROWS = 8
AHEAD = 3


def lane_table(sign):
    idx = np.arange(LANES)
    ang = 2.0 * np.pi * ((idx[:, None] * idx[None, :]) % LANES) / LANES
    c, s = np.cos(ang), sign * np.sin(ang)
    full = np.block([[c, s], [-s, c]])
    hi, lo = halves(full)
    return np.concatenate([hi, hi, lo], axis=0)


def doppler_table(pulses):
    part = pulses // RADIX
    m = np.arange(part)
    out = []
    for res in range(RADIX):
        ang = 2.0 * np.pi * ((m[None, :] * (RADIX * m[:, None] + res)) % pulses) / pulses
        c, s = np.cos(ang) / math.sqrt(pulses), -np.sin(ang) / math.sqrt(pulses)
        full = np.block([[c, -s], [s, c]])
        hi, lo = halves(full)
        out.append(np.concatenate([hi, lo], axis=1))
    return np.stack(out)


def split(x, axis):
    hi = x.astype(jnp.bfloat16)
    lo = (x - hi.astype(jnp.float32)).astype(jnp.bfloat16)
    return jnp.concatenate([hi, lo, hi], axis=axis)


def fft_list(re, im, sign):
    n = len(re)
    if n == 1:
        return re, im
    er, ei = fft_list(re[0::2], im[0::2], sign)
    odd_r, odd_i = fft_list(re[1::2], im[1::2], sign)
    half = n // 2
    out_r, out_i = [None] * n, [None] * n
    for k in range(half):
        a, b = odd_r[k], odd_i[k]
        if k == 0:
            tr, ti = a, b
        elif 4 * k == n:
            tr, ti = (b, -a) if sign < 0 else (-b, a)
        elif 8 * k == n or 8 * k == 3 * n:
            h = math.sqrt(0.5)
            c = h if 8 * k == n else -h
            tr = c * a - (sign * h) * b
            ti = c * b + (sign * h) * a
        else:
            c = math.cos(2.0 * math.pi * k / n)
            s = sign * math.sin(2.0 * math.pi * k / n)
            tr = c * a - s * b
            ti = s * a + c * b
        out_r[k], out_i[k] = er[k] + tr, ei[k] + ti
        out_r[k + half], out_i[k + half] = er[k] - tr, ei[k] - ti
    return out_r, out_i


def range_rows(xs, c, r0, tw8, rep8, wf, wi, comp):
    n, per = comp.shape[1], comp.shape[2]
    cols = n * per
    rows = pl.ds(r0, SUB)
    re = [xs[0, c, rows, a * LANES:(a + 1) * LANES].astype(jnp.float32) for a in range(cols)]
    im = [xs[1, c, rows, a * LANES:(a + 1) * LANES].astype(jnp.float32) for a in range(cols)]
    re, im = fft_list(re, im, -1.0)
    mr, mi = jnp.concatenate(re, axis=0), jnp.concatenate(im, axis=0)
    tr, ti = tw8[0], tw8[1]
    m = jnp.concatenate([mr * tr - mi * ti, mr * ti + mi * tr], axis=1)
    f = jnp.dot(split(m, 1), wf[...], preferred_element_type=jnp.float32)
    fr, fi = f[:, :LANES], f[:, LANES:]
    tr, ti = rep8[0], rep8[1]
    m = jnp.concatenate([fr * tr - fi * ti, fr * ti + fi * tr], axis=1)
    f = jnp.dot(split(m, 1), wi[...], preferred_element_type=jnp.float32)
    fr, fi = f[:, :LANES], f[:, LANES:]
    tr, ti = tw8[0], tw8[1]
    mr, mi = fr * tr + fi * ti, fi * tr - fr * ti
    re = [mr[a * SUB:(a + 1) * SUB] for a in range(cols)]
    im = [mi[a * SUB:(a + 1) * SUB] for a in range(cols)]
    re, im = fft_list(re, im, 1.0)
    for j in range(n):
        for a in range(per):
            comp[c, j, a, 0, rows, :] = re[j * per + a]
            comp[c, j, a, 1, rows, :] = im[j * per + a]


def doppler_chunk(recv, c, g, table, pw, hi_ref, lo_ref):
    quarter = recv.shape[3] // RADIX
    a, b, cc, d = ([recv[c, g, ri, q * quarter:(q + 1) * quarter, :] for ri in range(2)] for q in range(RADIX))
    sr, si = a[0] + cc[0], a[1] + cc[1]
    dr, di = a[0] - cc[0], a[1] - cc[1]
    ur, ui = b[0] + d[0], b[1] + d[1]
    vr, vi = b[0] - d[0], b[1] - d[1]
    ys = [(sr + ur, si + ui), (dr + vi, di - vr), (sr - ur, si - ui), (dr - vi, di + vr)]
    for res in range(RADIX):
        y = jnp.concatenate(ys[res], axis=0)
        near = y.astype(jnp.bfloat16)
        both = jnp.concatenate([near, (y - near.astype(jnp.float32)).astype(jnp.bfloat16)], axis=1)
        width = y.shape[0]
        main = jnp.dot(table[res, :, :width], both, preferred_element_type=jnp.float32)
        rest = jnp.dot(table[res, :, width:], near, preferred_element_type=jnp.float32)
        out = main[:, :LANES] + main[:, LANES:] + rest
        re, im = out[:quarter], out[quarter:]
        p = re * re + im * im
        hi = p.astype(jnp.bfloat16)
        pw[c, g, res] = p
        hi_ref[c, g + 1, res] = hi
        lo_ref[c, g + 1, res] = (p - hi.astype(jnp.float32)).astype(jnp.bfloat16)


def cfar_chunk(c, g, first_gate, gates, thresh, window, pw, hi_ref, lo_ref, band, stage, out, acc):
    quarter = pw.shape[3]
    total = RADIX * quarter
    parts = [ref[c, g + k].reshape(total, LANES) for ref in (hi_ref, lo_ref) for k in range(3)]
    noise = jnp.dot(jnp.concatenate(parts, axis=1), band[c], preferred_element_type=jnp.float32)
    guard = window[c, 0]
    reach = guard + window[c, 1]
    gate = first_gate + g * LANES + lax.broadcasted_iota(jnp.int32, (SUB, LANES), 1)
    after = gates - 1 - gate
    cells = jnp.minimum(gate, reach) - jnp.minimum(gate, guard) + jnp.minimum(after, reach) - jnp.minimum(after, guard)
    cells = cells.astype(jnp.float32)[:1]
    inv = thresh[c, 1].astype(jnp.float32) / thresh[c, 0].astype(jnp.float32)
    ratio = pw[c, g].reshape(total, LANES) * cells / (noise + EPSILON)
    for res in range(RADIX):
        stage[pl.ds(res, quarter, stride=RADIX), :] = ratio[res * quarter:(res + 1) * quarter]
    out[c, :, pl.ds(pl.multiple_of(g * LANES, LANES), LANES)] = stage[...]
    soft = jnp.clip(ratio * inv - 1.0, 0.0, 1.0)
    acc[...] += jnp.sum(soft.reshape(total // SUB, SUB, LANES), axis=0)


def kernel(sizes, rep_hbm, thresh_hbm, window_hbm, x_hbm, tw_hbm, wf_hbm, wi_hbm, t_hbm, out, count,
           rep, thresh, window, tw, nat, xs, wf, wi, table, tw8, rep8, comp, recv, pw, hi_ref, lo_ref, band, stage, pack, halo, gather, acc,
           in_sem, tab_sem, row_send, row_recv, chunk_send, chunk_recv, halo_send, halo_recv, sum_sem):
    n, nx, ns, rows = sizes
    _, channels, part, gates = xs.shape
    chunks = comp.shape[2]
    quarter = pw.shape[3]
    pulses = RADIX * quarter
    own = gates // n
    blocks = part // rows
    last = channels - 1
    z, x, s = lax.axis_index("pulse"), lax.axis_index("chan"), lax.axis_index("sub")
    peers = n * nx * ns
    me = (z * nx + x) * ns + s
    h = n // 2
    half = z // h

    def each(body, lo, hi):
        def run(i, carry):
            body(i)
            return carry
        lax.fori_loop(lo, hi, run, 0, unroll=hi - lo < 4)

    def beside(act):
        for ox in range(nx):
            for os in range(ns):
                if ox or os:
                    act({"pulse": z, "chan": lax.rem(x + ox, nx), "sub": lax.rem(s + os, ns)})

    def others(act):
        def along(o):
            for ox in range(nx):
                for os in range(ns):
                    act({"pulse": lax.rem(z + n - o, n), "chan": lax.rem(x + ox, nx), "sub": lax.rem(s + os, ns)})
        each(along, 1, n)
        beside(act)

    barrier = pltpu.get_barrier_semaphore()

    def load(b):
        c = b // blocks
        r = pl.ds(pl.multiple_of(lax.rem(b, blocks) * rows, rows), rows)
        return pltpu.make_async_copy(x_hbm.at[:, c, r, :], xs.at[:, c, r, :], in_sem.at[b])

    tables = [pltpu.make_async_copy(a, b, tab_sem.at[i])
              for i, (a, b) in enumerate(((rep_hbm, rep), (tw_hbm, tw), (wf_hbm, wf), (wi_hbm, wi), (t_hbm, table),
                                         (thresh_hbm, thresh), (window_hbm, window)))]
    tables[0].start()
    load(0).start()
    for copy in tables[1:4]:
        copy.start()
    def greet(who):
        pl.semaphore_signal(barrier, 1, device_id=who, device_id_type=MESH)

    each(lambda o: greet({"pulse": lax.rem(z + o, n)}), 1, n)
    beside(greet)
    for b in range(1, min(2, channels * blocks)):
        load(b).start()
    cols = tw.shape[1]
    nat[...] = jnp.zeros_like(nat)
    tables[0].wait()
    for ri in range(2):
        for k in range(cols):
            nat[ri * cols + k:ri * cols + k + 1, :] = rep[ri:ri + 1, k * LANES:(k + 1) * LANES]
    turned = jnp.transpose(nat[...])
    row = lax.broadcasted_iota(jnp.int32, (LANES, LANES), 0)
    lane = lax.broadcasted_iota(jnp.int32, (LANES, LANES), 1)
    per = LANES // cols
    pick = [jnp.where(jnp.logical_and(row >= ri * cols, lane == per * (row - ri * cols)), 1.0, 0.0) for ri in range(2)]
    pick = jnp.concatenate(pick, axis=1).astype(jnp.bfloat16)
    terms = []
    for _ in range(3):
        terms.append(turned.astype(jnp.bfloat16))
        turned = turned - terms[-1].astype(jnp.float32)
    placed = jnp.dot(jnp.concatenate(terms, axis=1), jnp.concatenate([pick] * 3, axis=0),
                     preferred_element_type=jnp.float32) * (INPUT_SCALE / gates)
    for ri in range(2):
        filt = placed[:cols, ri * LANES:(ri + 1) * LANES]
        for k in range(1, per):
            filt = filt + pltpu.roll(placed[k * cols:(k + 1) * cols, ri * LANES:(ri + 1) * LANES], k, 1)
        for k in range(cols):
            rep8[ri, k * SUB:(k + 1) * SUB, :] = jnp.broadcast_to(filt[k:k + 1, :], (SUB, LANES))
    tables[1].wait()
    for k in range(cols):
        for ri in range(2):
            tw8[ri, k * SUB:(k + 1) * SUB, :] = jnp.broadcast_to(tw[ri, k:k + 1, :], (SUB, LANES))

    def near(k):
        return half * h + lax.rem(lax.rem(z, h) + 1 + k, h)

    def cross(k):
        return (1 - half) * h + lax.rem(z + s + k, h)

    def row_copy(c, dest, b):
        r = pl.multiple_of(b * rows, rows)
        return pltpu.make_async_remote_copy(
            comp.at[c, dest, :, :, pl.ds(r, rows), :],
            recv.at[c, :, :, pl.ds(pl.multiple_of(z * part + r, rows), rows), :],
            row_send.at[c, dest], row_recv.at[c, z],
            device_id={"pulse": dest}, device_id_type=MESH)

    def row_all(c, dest, src):
        return pltpu.make_async_remote_copy(
            comp.at[c, dest], recv.at[c, :, :, pl.ds(pl.multiple_of(src * part, part), part), :],
            row_send.at[c, dest], row_recv.at[c, src],
            device_id={"pulse": dest}, device_id_type=MESH)

    def chunk_copy(dest, src, g):
        return pltpu.make_async_remote_copy(
            comp.at[last, dest, g], recv.at[last, g, :, pl.ds(pl.multiple_of(src * part, part), part), :],
            chunk_send.at[dest, g], chunk_recv.at[src, g],
            device_id={"pulse": dest}, device_id_type=MESH)

    outer = jnp.logical_and(n == 4, jnp.logical_or(z == 0, z == n - 1))

    def row_near(c, b):
        for k in range(h - 1):
            row_copy(c, near(k), b).start()

    def row_cross(c, b):
        for k in range(h):
            row_copy(c, cross(k), b).start()

    def step(b, carry):
        c = b // blocks
        r0 = lax.rem(b, blocks) * rows
        load(b).wait()

        @pl.when(b + 2 < channels * blocks)
        def _():
            load(b + 2).start()

        @pl.when(b == 0)
        def _():
            tables[2].wait()
            tables[3].wait()
            for copy in tables[4:]:
                copy.start()

        for u in range(rows // SUB):
            range_rows(xs, c, pl.multiple_of(r0 + u * SUB, SUB), tw8, rep8, wf, wi, comp)

        @pl.when(b == 0)
        def _():
            pl.semaphore_wait(barrier, n - 1 + nx * ns - 1)

        @pl.when(b < last * blocks)
        def _():
            pc, pb = c, lax.rem(b, blocks)

            @pl.when(outer)
            def _():
                row_near(pc, pb)

            @pl.when(jnp.logical_not(outer))
            def _():
                row_cross(pc, pb)

        return carry

    lax.fori_loop(0, channels * blocks, step, 0)

    def order(k):
        odd = lax.rem(k, 2)
        return odd * (chunks - 1) + (1 - 2 * odd) * (k // 2)

    def rest(t):
        c, b = t // blocks, lax.rem(t, blocks)

        @pl.when(outer)
        def _():
            row_cross(c, b)

        @pl.when(jnp.logical_not(outer))
        def _():
            row_near(c, b)

    def last_near(k):
        for q in range(h - 1):
            chunk_copy(near(q), z, order(k)).start()

    def far(q):
        return (2 - half) * h - 1 - q

    def last_cross(k):
        end = k // (chunks - 1) if chunks > 1 else 1
        for q in range(h):
            chunk_copy(end * far(q) + (1 - end) * cross(q), z, order(k)).start()

    ahead = min(AHEAD, chunks)
    each(last_near, 0, chunks)
    each(rest, 0, last * blocks)
    each(last_cross, 0, ahead)

    def keep(t):
        c, g = t // chunks, lax.rem(t, chunks)
        for ri in range(2):
            recv[c, g, ri, pl.ds(pl.multiple_of(z * part, part), part), :] = comp[c, z, g, ri]

    each(keep, 0, channels * chunks)
    for copy in tables[4:]:
        copy.wait()
    q = lax.broadcasted_iota(jnp.int32, (3 * LANES, LANES), 0)
    j = lax.broadcasted_iota(jnp.int32, (3 * LANES, LANES), 1)
    dist = jnp.abs(q - LANES - j)
    for c in range(channels):
        guard = window[c, 0]
        reach = guard + window[c, 1]
        inside = jnp.where(dist > guard, 1.0, 0.0) * jnp.where(dist <= reach, 1.0, 0.0)
        inside = inside.astype(jnp.bfloat16)
        band[c] = jnp.concatenate([inside, inside], axis=0)
        blank = jnp.zeros((RADIX, quarter, LANES), jnp.bfloat16)
        for ref in (hi_ref, lo_ref):
            ref[c, 0] = blank
            ref[c, chunks + 1] = blank
    acc[...] = jnp.zeros_like(acc)

    def dop(c, g):
        doppler_chunk(recv, c, g, table, pw, hi_ref, lo_ref)

    def cfar(c, g):
        cfar_chunk(c, g, z * own, gates, thresh, window, pw, hi_ref, lo_ref, band, stage, out, acc)

    def pack_left(c):
        pack[c, 0] = jnp.concatenate([pw[c, 0, res][:, :MARGIN] for res in range(RADIX)], axis=1)

    def pack_right(c):
        pack[c, 1] = jnp.concatenate([pw[c, chunks - 1, res][:, LANES - MARGIN:] for res in range(RADIX)], axis=1)

    def halo_copy(c, side, dest):
        return pltpu.make_async_remote_copy(
            pack.at[c, side], halo.at[c, 1 - side], halo_send.at[c, side], halo_recv.at[c, 1 - side],
            device_id={"pulse": dest}, device_id_type=MESH)

    def send_halo(c):
        @pl.when(z > 0)
        def _():
            halo_copy(c, 0, z - 1).start()

        @pl.when(z < n - 1)
        def _():
            halo_copy(c, 1, z + 1).start()

    def unpack(c, side):
        for res in range(RADIX):
            turn = (LANES - MARGIN - MARGIN * res if side == 0 else LANES - MARGIN * res) % LANES
            p = halo[c, side]
            if turn:
                p = pltpu.roll(p, turn, 1)
            hi = p.astype(jnp.bfloat16)
            at = 0 if side == 0 else chunks + 1
            hi_ref[c, at, res] = hi
            lo_ref[c, at, res] = (p - hi.astype(jnp.float32)).astype(jnp.bfloat16)

    def take_halo(c):
        @pl.when(z > 0)
        def _():
            halo_copy(c, 1, z).wait_recv()
            unpack(c, 0)

        @pl.when(z < n - 1)
        def _():
            halo_copy(c, 0, z).wait_recv()
            unpack(c, 1)

    for c in range(last):
        for o in range(1, n):
            row_all(c, z, lax.rem(z + o, n)).wait_recv()
        each(functools.partial(dop, c), 0, chunks)
        pack_left(c)
        pack_right(c)
        if chunks > 2:
            cfar(c, 1)
        send_halo(c)
        each(functools.partial(cfar, c), 2, chunks - 1)

    def arrive(k):
        for o in range(1, n):
            chunk_copy(z, lax.rem(z + o, n), order(k)).wait_recv()

    head = chunks - 1 if chunks >= 4 else chunks

    def last_step(k):
        @pl.when(k + ahead < chunks)
        def _():
            last_cross(k + ahead)

        arrive(k)
        dop(last, order(k))

        @pl.when(k == 0)
        def _():
            pack_left(last)

        @pl.when(k == min(1, chunks - 1))
        def _():
            pack_right(last)

        if chunks >= 4:
            @pl.when(k == 2)
            def _():
                send_halo(last)

            @pl.when(k >= 4)
            def _():
                cfar(last, order(k - 2))

    each(last_step, 0, head)
    if chunks < 4:
        send_halo(last)
        each(functools.partial(cfar, last), 1, chunks - 1)
    for c in range(channels):
        take_halo(c)
    edges = min(2, chunks)

    def edge(t):
        cfar(t // edges, lax.rem(t, edges) * (chunks - 1))

    each(edge, 0, channels * edges)
    if chunks >= 4:
        arrive(chunks - 1)
        dop(last, order(jnp.int32(chunks - 1)))
        for k in range(chunks - 3, chunks):
            cfar(last, (k % 2) * (chunks - 1) + (1 - 2 * (k % 2)) * (k // 2))

    gather[me] = jnp.sum(acc[...], axis=0, keepdims=True)
    for c in range(channels):
        @pl.when(z > 0)
        def _():
            halo_copy(c, 0, z - 1).wait_send()

        @pl.when(z < n - 1)
        def _():
            halo_copy(c, 1, z + 1).wait_send()

    def tell(who):
        pltpu.make_async_remote_copy(
            gather.at[me], gather.at[me], sum_sem.at[0], sum_sem.at[1],
            device_id=who, device_id_type=MESH).start()

    others(tell)
    for c in range(last):
        for o in range(1, n):
            row_all(c, lax.rem(z + o, n), z).wait_send()

    def sent(g):
        for o in range(1, n):
            chunk_copy(lax.rem(z + o, n), z, g).wait_send()

    each(sent, 0, chunks)
    every = pltpu.make_async_remote_copy(
        gather.at[pl.ds(0, peers - 1)], gather.at[pl.ds(0, peers - 1)], sum_sem.at[0], sum_sem.at[1],
        device_id={"pulse": lax.rem(z + 1, n)}, device_id_type=MESH)
    every.wait_recv()
    total = jnp.sum(gather[...], axis=0)
    total = jnp.sum(total, axis=1, keepdims=True) * (1024.0 / (pulses * gates))
    count[...] = jnp.broadcast_to(total, count.shape)
    every.wait_send()


def deliver_kernel(ratio, count, ratio_out, count_out, one, sem):
    channels, pulses, _ = ratio.shape
    step = pulses // 8
    one[0] = count[0, 0]
    copies = [pltpu.make_async_copy(one, count_out, sem.at[0])]
    for i in range(8 * channels):
        c, r = i // 8, pl.ds(i % 8 * step, step)
        copies.append(pltpu.make_async_copy(ratio.at[c, r], ratio_out.at[c, r], sem.at[i + 1]))
    for copy in copies:
        copy.start()
    for copy in copies:
        copy.wait()


def deliver(ratio, count):
    return pl.pallas_call(
        deliver_kernel,
        in_specs=[pl.BlockSpec(memory_space=pltpu.VMEM)] * 2,
        out_specs=[pl.BlockSpec(memory_space=pltpu.HBM)] * 2,
        out_shape=[jax.ShapeDtypeStruct(ratio.shape, jnp.float32), jax.ShapeDtypeStruct((1,), jnp.float32)],
        scratch_shapes=[pltpu.SMEM((1,), jnp.float32), pltpu.SemaphoreType.DMA((8 * ratio.shape[0] + 1,))],
        compiler_params=pltpu.CompilerParams(vmem_limit_bytes=1 << 20),
    )(*(pltpu.with_memory_space_constraint(a, pltpu.VMEM) for a in (ratio, count)))


def local(samples, replica, window, thresh):
    _, channels, part, gates = samples.shape
    n, nx, ns = (lax.axis_size(a) for a in ("pulse", "chan", "sub"))
    cols = gates // LANES
    pulses = part * n
    own = gates // n
    chunks = own // LANES
    quarter = pulses // RADIX
    rows = min(ROWS, part)
    k1 = np.arange(cols)[:, None]
    b = np.arange(LANES)[None, :]
    ang = 2.0 * np.pi * ((k1 * b) % gates) / gates
    tw = np.stack([np.cos(ang), -np.sin(ang)]).astype(np.float32)
    wf, wi = lane_table(-1.0), lane_table(1.0)
    table = doppler_table(pulses)
    peers = n * nx * ns
    f32, bf16 = jnp.float32, jnp.bfloat16
    vmem, hbm = (pl.BlockSpec(memory_space=m) for m in (pltpu.VMEM, pltpu.HBM))
    dma = pltpu.SemaphoreType.DMA
    return deliver(*pl.pallas_call(
        functools.partial(kernel, (n, nx, ns, rows)),
        in_specs=[hbm] * 8,
        out_specs=[vmem, vmem],
        out_shape=[pltpu.VMEM((channels, pulses, own), f32), pltpu.VMEM((1, LANES), f32)],
        scratch_shapes=[
            pltpu.VMEM(replica.shape, f32),
            pltpu.SMEM(thresh.shape, jnp.int32),
            pltpu.SMEM(window.shape, jnp.int32),
            pltpu.VMEM(tw.shape, f32),
            pltpu.VMEM((LANES, LANES), f32),
            pltpu.VMEM((2, channels, part, gates), jnp.int32),
            pltpu.VMEM(wf.shape, bf16),
            pltpu.VMEM(wi.shape, bf16),
            pltpu.VMEM(table.shape, bf16),
            pltpu.VMEM((2, cols * SUB, LANES), f32),
            pltpu.VMEM((2, cols * SUB, LANES), f32),
            pltpu.VMEM((channels, n, chunks, 2, part, LANES), f32),
            pltpu.VMEM((channels, chunks, 2, pulses, LANES), f32),
            pltpu.VMEM((channels, chunks, RADIX, quarter, LANES), f32),
            pltpu.VMEM((channels, chunks + 2, RADIX, quarter, LANES), bf16),
            pltpu.VMEM((channels, chunks + 2, RADIX, quarter, LANES), bf16),
            pltpu.VMEM((channels, 6 * LANES, LANES), bf16),
            pltpu.VMEM((pulses, LANES), f32),
            pltpu.VMEM((channels, 2, quarter, LANES), f32),
            pltpu.VMEM((channels, 2, quarter, LANES), f32),
            pltpu.VMEM((peers, 1, LANES), f32),
            pltpu.VMEM((SUB, LANES), f32),
            dma((channels * (part // rows),)),
            dma((7,)),
            dma((channels, n)),
            dma((channels, n)),
            dma((n, chunks)),
            dma((n, chunks)),
            dma((channels, 2)),
            dma((channels, 2)),
            dma((2,)),
        ],
        compiler_params=pltpu.CompilerParams(
            collective_id=0, has_side_effects=True, vmem_limit_bytes=48 << 20),
        cost_estimate=pl.CostEstimate(flops=int(2e10), bytes_accessed=32 << 20, transcendentals=0),
    )(*(pltpu.with_memory_space_constraint(jnp.asarray(a), pltpu.HBM)
        for a in (replica, thresh, window, samples, tw, wf, wi, table))))


def solution(mesh):
    in_specs = (
        P(None, ("grp", "chan", "sub"), "pulse", None),
        P(),
        P(("grp", "chan", "sub"), None),
        P(("grp", "chan", "sub"), None),
    )
    out_specs = (P(("grp", "chan", "sub"), None, "pulse"), P("grp"))
    return jax.shard_map(lambda *a: tuple(local(*a)), mesh=mesh, in_specs=in_specs, out_specs=out_specs, check_vma=False)
```

```python
import functools
import math

import jax
import jax.numpy as jnp
import numpy as np
from jax import lax
from jax.experimental import pallas as pl
from jax.experimental.pallas import tpu as pltpu
from jax.sharding import PartitionSpec as P

GUARD_MAX = 4
TRAIN_MAX = 28
MARGIN = GUARD_MAX + TRAIN_MAX
EPSILON = 1e-06
INPUT_SCALE = 1.0 / 2048.0
LANES = 128
SUB = 8
RADIX = 4


def halves(table):
    hi = np.asarray(table, np.float32).astype(jnp.bfloat16)
    lo = (np.asarray(table, np.float64) - hi.astype(np.float64)).astype(jnp.bfloat16)
    return hi, lo


MESH = pl.DeviceIdType.MESH
ROWS = 8
AHEAD = 3


def lane_table(sign):
    idx = np.arange(LANES)
    ang = 2.0 * np.pi * ((idx[:, None] * idx[None, :]) % LANES) / LANES
    c, s = np.cos(ang), sign * np.sin(ang)
    full = np.block([[c, s], [-s, c]])
    hi, lo = halves(full)
    return np.concatenate([hi, hi, lo], axis=0)


def doppler_table(pulses):
    part = pulses // RADIX
    m = np.arange(part)
    out = []
    for res in range(RADIX):
        ang = 2.0 * np.pi * ((m[None, :] * (RADIX * m[:, None] + res)) % pulses) / pulses
        c, s = np.cos(ang) / math.sqrt(pulses), -np.sin(ang) / math.sqrt(pulses)
        full = np.block([[c, -s], [s, c]])
        hi, lo = halves(full)
        out.append(np.concatenate([hi, lo], axis=1))
    return np.stack(out)


def split(x, axis):
    hi = x.astype(jnp.bfloat16)
    lo = (x - hi.astype(jnp.float32)).astype(jnp.bfloat16)
    return jnp.concatenate([hi, lo, hi], axis=axis)


def fft_list(re, im, sign):
    n = len(re)
    if n == 1:
        return re, im
    er, ei = fft_list(re[0::2], im[0::2], sign)
    odd_r, odd_i = fft_list(re[1::2], im[1::2], sign)
    half = n // 2
    out_r, out_i = [None] * n, [None] * n
    for k in range(half):
        a, b = odd_r[k], odd_i[k]
        if k == 0:
            tr, ti = a, b
        elif 4 * k == n:
            tr, ti = (b, -a) if sign < 0 else (-b, a)
        elif 8 * k == n or 8 * k == 3 * n:
            h = math.sqrt(0.5)
            c = h if 8 * k == n else -h
            tr = c * a - (sign * h) * b
            ti = c * b + (sign * h) * a
        else:
            c = math.cos(2.0 * math.pi * k / n)
            s = sign * math.sin(2.0 * math.pi * k / n)
            tr = c * a - s * b
            ti = s * a + c * b
        out_r[k], out_i[k] = er[k] + tr, ei[k] + ti
        out_r[k + half], out_i[k + half] = er[k] - tr, ei[k] - ti
    return out_r, out_i


def range_rows(xs, c, r0, tw8, rep8, wf, wi, comp):
    n, per = comp.shape[1], comp.shape[2]
    cols = n * per
    rows = pl.ds(r0, SUB)
    re = [xs[0, c, rows, a * LANES:(a + 1) * LANES].astype(jnp.float32) for a in range(cols)]
    im = [xs[1, c, rows, a * LANES:(a + 1) * LANES].astype(jnp.float32) for a in range(cols)]
    re, im = fft_list(re, im, -1.0)
    mr, mi = jnp.concatenate(re, axis=0), jnp.concatenate(im, axis=0)
    tr, ti = tw8[0], tw8[1]
    m = jnp.concatenate([mr * tr - mi * ti, mr * ti + mi * tr], axis=1)
    f = jnp.dot(split(m, 1), wf[...], preferred_element_type=jnp.float32)
    fr, fi = f[:, :LANES], f[:, LANES:]
    tr, ti = rep8[0], rep8[1]
    m = jnp.concatenate([fr * tr - fi * ti, fr * ti + fi * tr], axis=1)
    f = jnp.dot(split(m, 1), wi[...], preferred_element_type=jnp.float32)
    fr, fi = f[:, :LANES], f[:, LANES:]
    tr, ti = tw8[0], tw8[1]
    mr, mi = fr * tr + fi * ti, fi * tr - fr * ti
    re = [mr[a * SUB:(a + 1) * SUB] for a in range(cols)]
    im = [mi[a * SUB:(a + 1) * SUB] for a in range(cols)]
    re, im = fft_list(re, im, 1.0)
    for j in range(n):
        for a in range(per):
            comp[c, j, a, 0, rows, :] = re[j * per + a]
            comp[c, j, a, 1, rows, :] = im[j * per + a]


def doppler_chunk(recv, c, g, table, pw, hi_ref, lo_ref):
    quarter = recv.shape[3] // RADIX
    a, b, cc, d = ([recv[c, g, ri, q * quarter:(q + 1) * quarter, :] for ri in range(2)] for q in range(RADIX))
    sr, si = a[0] + cc[0], a[1] + cc[1]
    dr, di = a[0] - cc[0], a[1] - cc[1]
    ur, ui = b[0] + d[0], b[1] + d[1]
    vr, vi = b[0] - d[0], b[1] - d[1]
    ys = [(sr + ur, si + ui), (dr + vi, di - vr), (sr - ur, si - ui), (dr - vi, di + vr)]
    for res in range(RADIX):
        y = jnp.concatenate(ys[res], axis=0)
        near = y.astype(jnp.bfloat16)
        both = jnp.concatenate([near, (y - near.astype(jnp.float32)).astype(jnp.bfloat16)], axis=1)
        width = y.shape[0]
        main = jnp.dot(table[res, :, :width], both, preferred_element_type=jnp.float32)
        rest = jnp.dot(table[res, :, width:], near, preferred_element_type=jnp.float32)
        out = main[:, :LANES] + main[:, LANES:] + rest
        re, im = out[:quarter], out[quarter:]
        p = re * re + im * im
        hi = p.astype(jnp.bfloat16)
        pw[c, g, res] = p
        hi_ref[c, g + 1, res] = hi
        lo_ref[c, g + 1, res] = (p - hi.astype(jnp.float32)).astype(jnp.bfloat16)


def cfar_chunk(c, g, first_gate, gates, thresh, window, pw, hi_ref, lo_ref, band, stage, out, acc):
    quarter = pw.shape[3]
    total = RADIX * quarter
    parts = [ref[c, g + k].reshape(total, LANES) for ref in (hi_ref, lo_ref) for k in range(3)]
    noise = jnp.dot(jnp.concatenate(parts, axis=1), band[c], preferred_element_type=jnp.float32)
    guard = window[c, 0]
    reach = guard + window[c, 1]
    gate = first_gate + g * LANES + lax.broadcasted_iota(jnp.int32, (SUB, LANES), 1)
    after = gates - 1 - gate
    cells = jnp.minimum(gate, reach) - jnp.minimum(gate, guard) + jnp.minimum(after, reach) - jnp.minimum(after, guard)
    cells = cells.astype(jnp.float32)[:1]
    inv = thresh[c, 1].astype(jnp.float32) / thresh[c, 0].astype(jnp.float32)
    ratio = pw[c, g].reshape(total, LANES) * cells / (noise + EPSILON)
    for res in range(RADIX):
        stage[pl.ds(res, quarter, stride=RADIX), :] = ratio[res * quarter:(res + 1) * quarter]
    out[c, :, pl.ds(pl.multiple_of(g * LANES, LANES), LANES)] = stage[...]
    soft = jnp.clip(ratio * inv - 1.0, 0.0, 1.0)
    acc[...] += jnp.sum(soft.reshape(total // SUB, SUB, LANES), axis=0)


def kernel(sizes, rep_hbm, thresh_hbm, window_hbm, x_hbm, tw_hbm, wf_hbm, wi_hbm, t_hbm, out, count,
           rep, thresh, window, tw, nat, xs, wf, wi, table, tw8, rep8, comp, recv, pw, hi_ref, lo_ref, band, stage, pack, halo, gather, acc,
           in_sem, tab_sem, row_send, row_recv, chunk_send, chunk_recv, halo_send, halo_recv, sum_sem):
    n, nx, ns, rows = sizes
    _, channels, part, gates = xs.shape
    chunks = comp.shape[2]
    quarter = pw.shape[3]
    pulses = RADIX * quarter
    own = gates // n
    blocks = part // rows
    last = channels - 1
    z, x, s = lax.axis_index("pulse"), lax.axis_index("chan"), lax.axis_index("sub")
    peers = n * nx * ns
    me = (z * nx + x) * ns + s
    h = n // 2
    half = z // h

    def each(body, lo, hi):
        def run(i, carry):
            body(i)
            return carry
        lax.fori_loop(lo, hi, run, 0, unroll=hi - lo < 4)

    def beside(act):
        for ox in range(nx):
            for os in range(ns):
                if ox or os:
                    act({"pulse": z, "chan": lax.rem(x + ox, nx), "sub": lax.rem(s + os, ns)})

    def others(act):
        def along(o):
            for ox in range(nx):
                for os in range(ns):
                    act({"pulse": lax.rem(z + n - o, n), "chan": lax.rem(x + ox, nx), "sub": lax.rem(s + os, ns)})
        each(along, 1, n)
        beside(act)

    barrier = pltpu.get_barrier_semaphore()

    def load(b):
        c = b // blocks
        r = pl.ds(pl.multiple_of(lax.rem(b, blocks) * rows, rows), rows)
        return pltpu.make_async_copy(x_hbm.at[:, c, r, :], xs.at[:, c, r, :], in_sem.at[b])

    tables = [pltpu.make_async_copy(a, b, tab_sem.at[i])
              for i, (a, b) in enumerate(((rep_hbm, rep), (tw_hbm, tw), (wf_hbm, wf), (wi_hbm, wi), (t_hbm, table),
                                         (thresh_hbm, thresh), (window_hbm, window)))]
    tables[0].start()
    load(0).start()
    for copy in tables[1:4]:
        copy.start()
    def greet(who):
        pl.semaphore_signal(barrier, 1, device_id=who, device_id_type=MESH)

    each(lambda o: greet({"pulse": lax.rem(z + o, n)}), 1, n)
    beside(greet)
    for b in range(1, min(2, channels * blocks)):
        load(b).start()
    cols = tw.shape[1]
    nat[...] = jnp.zeros_like(nat)
    tables[0].wait()
    for ri in range(2):
        for k in range(cols):
            nat[ri * cols + k:ri * cols + k + 1, :] = rep[ri:ri + 1, k * LANES:(k + 1) * LANES]
    turned = jnp.transpose(nat[...])
    row = lax.broadcasted_iota(jnp.int32, (LANES, LANES), 0)
    lane = lax.broadcasted_iota(jnp.int32, (LANES, LANES), 1)
    per = LANES // cols
    pick = [jnp.where(jnp.logical_and(row >= ri * cols, lane == per * (row - ri * cols)), 1.0, 0.0) for ri in range(2)]
    pick = jnp.concatenate(pick, axis=1).astype(jnp.bfloat16)
    terms = []
    for _ in range(3):
        terms.append(turned.astype(jnp.bfloat16))
        turned = turned - terms[-1].astype(jnp.float32)
    placed = jnp.dot(jnp.concatenate(terms, axis=1), jnp.concatenate([pick] * 3, axis=0),
                     preferred_element_type=jnp.float32) * (INPUT_SCALE / gates)
    for ri in range(2):
        filt = placed[:cols, ri * LANES:(ri + 1) * LANES]
        for k in range(1, per):
            filt = filt + pltpu.roll(placed[k * cols:(k + 1) * cols, ri * LANES:(ri + 1) * LANES], k, 1)
        for k in range(cols):
            rep8[ri, k * SUB:(k + 1) * SUB, :] = jnp.broadcast_to(filt[k:k + 1, :], (SUB, LANES))
    tables[1].wait()
    for k in range(cols):
        for ri in range(2):
            tw8[ri, k * SUB:(k + 1) * SUB, :] = jnp.broadcast_to(tw[ri, k:k + 1, :], (SUB, LANES))

    def near(k):
        return half * h + lax.rem(lax.rem(z, h) + 1 + k, h)

    def cross(k):
        return (1 - half) * h + lax.rem(z + s + k, h)

    def row_copy(c, dest, b):
        r = pl.multiple_of(b * rows, rows)
        return pltpu.make_async_remote_copy(
            comp.at[c, dest, :, :, pl.ds(r, rows), :],
            recv.at[c, :, :, pl.ds(pl.multiple_of(z * part + r, rows), rows), :],
            row_send.at[c, dest], row_recv.at[c, z],
            device_id={"pulse": dest}, device_id_type=MESH)

    def row_all(c, dest, src):
        return pltpu.make_async_remote_copy(
            comp.at[c, dest], recv.at[c, :, :, pl.ds(pl.multiple_of(src * part, part), part), :],
            row_send.at[c, dest], row_recv.at[c, src],
            device_id={"pulse": dest}, device_id_type=MESH)

    def chunk_copy(dest, src, g):
        return pltpu.make_async_remote_copy(
            comp.at[last, dest, g], recv.at[last, g, :, pl.ds(pl.multiple_of(src * part, part), part), :],
            chunk_send.at[dest, g], chunk_recv.at[src, g],
            device_id={"pulse": dest}, device_id_type=MESH)

    outer = jnp.logical_and(n == 4, jnp.logical_or(z == 0, z == n - 1))

    def row_near(c, b):
        for k in range(h - 1):
            row_copy(c, near(k), b).start()

    def row_cross(c, b):
        for k in range(h):
            row_copy(c, cross(k), b).start()

    def step(b, carry):
        c = b // blocks
        r0 = lax.rem(b, blocks) * rows
        load(b).wait()

        @pl.when(b + 2 < channels * blocks)
        def _():
            load(b + 2).start()

        @pl.when(b == 0)
        def _():
            tables[2].wait()
            tables[3].wait()
            for copy in tables[4:]:
                copy.start()

        for u in range(rows // SUB):
            range_rows(xs, c, pl.multiple_of(r0 + u * SUB, SUB), tw8, rep8, wf, wi, comp)

        @pl.when(b == 0)
        def _():
            pl.semaphore_wait(barrier, n - 1 + nx * ns - 1)

        @pl.when(b < last * blocks)
        def _():
            pc, pb = c, lax.rem(b, blocks)

            @pl.when(outer)
            def _():
                row_near(pc, pb)

            @pl.when(jnp.logical_not(outer))
            def _():
                row_cross(pc, pb)

        return carry

    lax.fori_loop(0, channels * blocks, step, 0)

    def order(k):
        odd = lax.rem(k, 2)
        return odd * (chunks - 1) + (1 - 2 * odd) * (k // 2)

    def rest(t):
        c, b = t // blocks, lax.rem(t, blocks)

        @pl.when(outer)
        def _():
            row_cross(c, b)

        @pl.when(jnp.logical_not(outer))
        def _():
            row_near(c, b)

    def last_near(k):
        for q in range(h - 1):
            chunk_copy(near(q), z, order(k)).start()

    def far(q):
        return (1 - half) * (n - 1 - q) + half * q

    def last_cross(k):
        end = k // (chunks - 1) if chunks > 1 else 1
        for q in range(h):
            chunk_copy(end * far(q) + (1 - end) * cross(q), z, order(k)).start()

    ahead = min(AHEAD, chunks)
    each(last_near, 0, chunks)
    each(rest, 0, last * blocks)
    each(last_cross, 0, ahead)

    def keep(t):
        c, g = t // chunks, lax.rem(t, chunks)
        for ri in range(2):
            recv[c, g, ri, pl.ds(pl.multiple_of(z * part, part), part), :] = comp[c, z, g, ri]

    each(keep, 0, channels * chunks)
    for copy in tables[4:]:
        copy.wait()
    q = lax.broadcasted_iota(jnp.int32, (3 * LANES, LANES), 0)
    j = lax.broadcasted_iota(jnp.int32, (3 * LANES, LANES), 1)
    dist = jnp.abs(q - LANES - j)
    for c in range(channels):
        guard = window[c, 0]
        reach = guard + window[c, 1]
        inside = jnp.where(dist > guard, 1.0, 0.0) * jnp.where(dist <= reach, 1.0, 0.0)
        inside = inside.astype(jnp.bfloat16)
        band[c] = jnp.concatenate([inside, inside], axis=0)
        blank = jnp.zeros((RADIX, quarter, LANES), jnp.bfloat16)
        for ref in (hi_ref, lo_ref):
            ref[c, 0] = blank
            ref[c, chunks + 1] = blank
    acc[...] = jnp.zeros_like(acc)

    def dop(c, g):
        doppler_chunk(recv, c, g, table, pw, hi_ref, lo_ref)

    def cfar(c, g):
        cfar_chunk(c, g, z * own, gates, thresh, window, pw, hi_ref, lo_ref, band, stage, out, acc)

    def pack_left(c):
        pack[c, 0] = jnp.concatenate([pw[c, 0, res][:, :MARGIN] for res in range(RADIX)], axis=1)

    def pack_right(c):
        pack[c, 1] = jnp.concatenate([pw[c, chunks - 1, res][:, LANES - MARGIN:] for res in range(RADIX)], axis=1)

    def halo_copy(c, side, dest):
        return pltpu.make_async_remote_copy(
            pack.at[c, side], halo.at[c, 1 - side], halo_send.at[c, side], halo_recv.at[c, 1 - side],
            device_id={"pulse": dest}, device_id_type=MESH)

    def send_halo(c):
        @pl.when(z > 0)
        def _():
            halo_copy(c, 0, z - 1).start()

        @pl.when(z < n - 1)
        def _():
            halo_copy(c, 1, z + 1).start()

    def unpack(c, side):
        for res in range(RADIX):
            turn = (LANES - MARGIN - MARGIN * res if side == 0 else LANES - MARGIN * res) % LANES
            p = halo[c, side]
            if turn:
                p = pltpu.roll(p, turn, 1)
            hi = p.astype(jnp.bfloat16)
            at = 0 if side == 0 else chunks + 1
            hi_ref[c, at, res] = hi
            lo_ref[c, at, res] = (p - hi.astype(jnp.float32)).astype(jnp.bfloat16)

    def take_halo(c):
        @pl.when(z > 0)
        def _():
            halo_copy(c, 1, z).wait_recv()
            unpack(c, 0)

        @pl.when(z < n - 1)
        def _():
            halo_copy(c, 0, z).wait_recv()
            unpack(c, 1)

    for c in range(last):
        for o in range(1, n):
            row_all(c, z, lax.rem(z + o, n)).wait_recv()
        each(functools.partial(dop, c), 0, chunks)
        pack_left(c)
        pack_right(c)
        if chunks > 2:
            cfar(c, 1)
        send_halo(c)
        each(functools.partial(cfar, c), 2, chunks - 1)

    def arrive(k):
        for o in range(1, n):
            chunk_copy(z, lax.rem(z + o, n), order(k)).wait_recv()

    head = chunks - 1 if chunks >= 4 else chunks

    def last_step(k):
        @pl.when(k + ahead < chunks)
        def _():
            last_cross(k + ahead)

        arrive(k)
        dop(last, order(k))

        @pl.when(k == 0)
        def _():
            pack_left(last)

        @pl.when(k == min(1, chunks - 1))
        def _():
            pack_right(last)

        if chunks >= 4:
            @pl.when(k == 2)
            def _():
                send_halo(last)

            @pl.when(k >= 4)
            def _():
                cfar(last, order(k - 2))

    each(last_step, 0, head)
    if chunks < 4:
        send_halo(last)
        each(functools.partial(cfar, last), 1, chunks - 1)
    for c in range(channels):
        take_halo(c)
    edges = min(2, chunks)

    def edge(t):
        cfar(t // edges, lax.rem(t, edges) * (chunks - 1))

    each(edge, 0, channels * edges)
    if chunks >= 4:
        arrive(chunks - 1)
        dop(last, order(jnp.int32(chunks - 1)))
        for k in range(chunks - 3, chunks):
            cfar(last, (k % 2) * (chunks - 1) + (1 - 2 * (k % 2)) * (k // 2))

    gather[me] = jnp.sum(acc[...], axis=0, keepdims=True)
    for c in range(channels):
        @pl.when(z > 0)
        def _():
            halo_copy(c, 0, z - 1).wait_send()

        @pl.when(z < n - 1)
        def _():
            halo_copy(c, 1, z + 1).wait_send()

    def tell(who):
        pltpu.make_async_remote_copy(
            gather.at[me], gather.at[me], sum_sem.at[0], sum_sem.at[1],
            device_id=who, device_id_type=MESH).start()

    others(tell)
    for c in range(last):
        for o in range(1, n):
            row_all(c, lax.rem(z + o, n), z).wait_send()

    def sent(g):
        for o in range(1, n):
            chunk_copy(lax.rem(z + o, n), z, g).wait_send()

    each(sent, 0, chunks)
    every = pltpu.make_async_remote_copy(
        gather.at[pl.ds(0, peers - 1)], gather.at[pl.ds(0, peers - 1)], sum_sem.at[0], sum_sem.at[1],
        device_id={"pulse": lax.rem(z + 1, n)}, device_id_type=MESH)
    every.wait_recv()
    total = jnp.sum(gather[...], axis=0)
    total = jnp.sum(total, axis=1, keepdims=True) * (1024.0 / (pulses * gates))
    count[...] = jnp.broadcast_to(total, count.shape)
    every.wait_send()


def deliver_kernel(ratio, count, ratio_out, count_out, one, sem):
    channels, pulses, _ = ratio.shape
    step = pulses // 8
    copies = []
    for i in range(8 * channels):
        c, r = i // 8, pl.ds(i % 8 * step, step)
        copies.append(pltpu.make_async_copy(ratio.at[c, r], ratio_out.at[c, r], sem.at[i + 1]))
    for copy in copies:
        copy.start()
    one[0] = count[0, 0]
    copies.append(pltpu.make_async_copy(one, count_out, sem.at[0]))
    copies[-1].start()
    for copy in copies:
        copy.wait()


def deliver(ratio, count):
    return pl.pallas_call(
        deliver_kernel,
        in_specs=[pl.BlockSpec(memory_space=pltpu.VMEM)] * 2,
        out_specs=[pl.BlockSpec(memory_space=pltpu.HBM)] * 2,
        out_shape=[jax.ShapeDtypeStruct(ratio.shape, jnp.float32), jax.ShapeDtypeStruct((1,), jnp.float32)],
        scratch_shapes=[pltpu.SMEM((1,), jnp.float32), pltpu.SemaphoreType.DMA((8 * ratio.shape[0] + 1,))],
        compiler_params=pltpu.CompilerParams(vmem_limit_bytes=1 << 20),
    )(*(pltpu.with_memory_space_constraint(a, pltpu.VMEM) for a in (ratio, count)))


def local(samples, replica, window, thresh):
    _, channels, part, gates = samples.shape
    n, nx, ns = (lax.axis_size(a) for a in ("pulse", "chan", "sub"))
    cols = gates // LANES
    pulses = part * n
    own = gates // n
    chunks = own // LANES
    quarter = pulses // RADIX
    rows = min(ROWS, part)
    k1 = np.arange(cols)[:, None]
    b = np.arange(LANES)[None, :]
    ang = 2.0 * np.pi * ((k1 * b) % gates) / gates
    tw = np.stack([np.cos(ang), -np.sin(ang)]).astype(np.float32)
    wf, wi = lane_table(-1.0), lane_table(1.0)
    table = doppler_table(pulses)
    peers = n * nx * ns
    f32, bf16 = jnp.float32, jnp.bfloat16
    vmem, hbm = (pl.BlockSpec(memory_space=m) for m in (pltpu.VMEM, pltpu.HBM))
    dma = pltpu.SemaphoreType.DMA
    return deliver(*pl.pallas_call(
        functools.partial(kernel, (n, nx, ns, rows)),
        in_specs=[hbm] * 8,
        out_specs=[vmem, vmem],
        out_shape=[pltpu.VMEM((channels, pulses, own), f32), pltpu.VMEM((1, LANES), f32)],
        scratch_shapes=[
            pltpu.VMEM(replica.shape, f32),
            pltpu.SMEM(thresh.shape, jnp.int32),
            pltpu.SMEM(window.shape, jnp.int32),
            pltpu.VMEM(tw.shape, f32),
            pltpu.VMEM((LANES, LANES), f32),
            pltpu.VMEM((2, channels, part, gates), jnp.int32),
            pltpu.VMEM(wf.shape, bf16),
            pltpu.VMEM(wi.shape, bf16),
            pltpu.VMEM(table.shape, bf16),
            pltpu.VMEM((2, cols * SUB, LANES), f32),
            pltpu.VMEM((2, cols * SUB, LANES), f32),
            pltpu.VMEM((channels, n, chunks, 2, part, LANES), f32),
            pltpu.VMEM((channels, chunks, 2, pulses, LANES), f32),
            pltpu.VMEM((channels, chunks, RADIX, quarter, LANES), f32),
            pltpu.VMEM((channels, chunks + 2, RADIX, quarter, LANES), bf16),
            pltpu.VMEM((channels, chunks + 2, RADIX, quarter, LANES), bf16),
            pltpu.VMEM((channels, 6 * LANES, LANES), bf16),
            pltpu.VMEM((pulses, LANES), f32),
            pltpu.VMEM((channels, 2, quarter, LANES), f32),
            pltpu.VMEM((channels, 2, quarter, LANES), f32),
            pltpu.VMEM((peers, 1, LANES), f32),
            pltpu.VMEM((SUB, LANES), f32),
            dma((channels * (part // rows),)),
            dma((7,)),
            dma((channels, n)),
            dma((channels, n)),
            dma((n, chunks)),
            dma((n, chunks)),
            dma((channels, 2)),
            dma((channels, 2)),
            dma((2,)),
        ],
        compiler_params=pltpu.CompilerParams(
            collective_id=0, has_side_effects=True, vmem_limit_bytes=48 << 20),
        cost_estimate=pl.CostEstimate(flops=int(2e10), bytes_accessed=32 << 20, transcendentals=0),
    )(*(pltpu.with_memory_space_constraint(jnp.asarray(a), pltpu.HBM)
        for a in (replica, thresh, window, samples, tw, wf, wi, table))))


def solution(mesh):
    in_specs = (
        P(None, ("grp", "chan", "sub"), "pulse", None),
        P(),
        P(("grp", "chan", "sub"), None),
        P(("grp", "chan", "sub"), None),
    )
    out_specs = (P(("grp", "chan", "sub"), None, "pulse"), P("grp"))
    return jax.shard_map(lambda *a: tuple(local(*a)), mesh=mesh, in_specs=in_specs, out_specs=out_specs, check_vma=False)
```

```python
import functools
import math

import jax
import jax.numpy as jnp
import numpy as np
from jax import lax
from jax.experimental import pallas as pl
from jax.experimental.pallas import tpu as pltpu
from jax.sharding import PartitionSpec as P

GUARD_MAX = 4
TRAIN_MAX = 28
MARGIN = GUARD_MAX + TRAIN_MAX
EPSILON = 1e-06
INPUT_SCALE = 1.0 / 2048.0
LANES = 128
SUB = 8
RADIX = 4


def halves(table):
    hi = np.asarray(table, np.float32).astype(jnp.bfloat16)
    lo = (np.asarray(table, np.float64) - hi.astype(np.float64)).astype(jnp.bfloat16)
    return hi, lo


MESH = pl.DeviceIdType.MESH
ROWS = 8
AHEAD = 3


def lane_table(sign):
    idx = np.arange(LANES)
    ang = 2.0 * np.pi * ((idx[:, None] * idx[None, :]) % LANES) / LANES
    c, s = np.cos(ang), sign * np.sin(ang)
    full = np.block([[c, s], [-s, c]])
    hi, lo = halves(full)
    return np.concatenate([hi, hi, lo], axis=0)


def doppler_table(pulses):
    part = pulses // RADIX
    m = np.arange(part)
    out = []
    for res in range(RADIX):
        ang = 2.0 * np.pi * ((m[None, :] * (RADIX * m[:, None] + res)) % pulses) / pulses
        c, s = np.cos(ang) / math.sqrt(pulses), -np.sin(ang) / math.sqrt(pulses)
        full = np.block([[c, -s], [s, c]])
        hi, lo = halves(full)
        out.append(np.concatenate([hi, lo], axis=1))
    return np.stack(out)


def split(x, axis):
    hi = x.astype(jnp.bfloat16)
    lo = (x - hi.astype(jnp.float32)).astype(jnp.bfloat16)
    return jnp.concatenate([hi, lo, hi], axis=axis)


def fft_list(re, im, sign):
    n = len(re)
    if n == 1:
        return re, im
    er, ei = fft_list(re[0::2], im[0::2], sign)
    odd_r, odd_i = fft_list(re[1::2], im[1::2], sign)
    half = n // 2
    out_r, out_i = [None] * n, [None] * n
    for k in range(half):
        a, b = odd_r[k], odd_i[k]
        if k == 0:
            tr, ti = a, b
        elif 4 * k == n:
            tr, ti = (b, -a) if sign < 0 else (-b, a)
        elif 8 * k == n or 8 * k == 3 * n:
            h = math.sqrt(0.5)
            c = h if 8 * k == n else -h
            tr = c * a - (sign * h) * b
            ti = c * b + (sign * h) * a
        else:
            c = math.cos(2.0 * math.pi * k / n)
            s = sign * math.sin(2.0 * math.pi * k / n)
            tr = c * a - s * b
            ti = s * a + c * b
        out_r[k], out_i[k] = er[k] + tr, ei[k] + ti
        out_r[k + half], out_i[k + half] = er[k] - tr, ei[k] - ti
    return out_r, out_i


def range_rows(xs, c, r0, tw8, rep8, wf, wi, comp):
    n, per = comp.shape[1], comp.shape[2]
    cols = n * per
    rows = pl.ds(r0, SUB)
    re = [xs[0, c, rows, a * LANES:(a + 1) * LANES].astype(jnp.float32) for a in range(cols)]
    im = [xs[1, c, rows, a * LANES:(a + 1) * LANES].astype(jnp.float32) for a in range(cols)]
    re, im = fft_list(re, im, -1.0)
    mr, mi = jnp.concatenate(re, axis=0), jnp.concatenate(im, axis=0)
    tr, ti = tw8[0], tw8[1]
    m = jnp.concatenate([mr * tr - mi * ti, mr * ti + mi * tr], axis=1)
    f = jnp.dot(split(m, 1), wf[...], preferred_element_type=jnp.float32)
    fr, fi = f[:, :LANES], f[:, LANES:]
    tr, ti = rep8[0], rep8[1]
    m = jnp.concatenate([fr * tr - fi * ti, fr * ti + fi * tr], axis=1)
    f = jnp.dot(split(m, 1), wi[...], preferred_element_type=jnp.float32)
    fr, fi = f[:, :LANES], f[:, LANES:]
    tr, ti = tw8[0], tw8[1]
    mr, mi = fr * tr + fi * ti, fi * tr - fr * ti
    re = [mr[a * SUB:(a + 1) * SUB] for a in range(cols)]
    im = [mi[a * SUB:(a + 1) * SUB] for a in range(cols)]
    re, im = fft_list(re, im, 1.0)
    for j in range(n):
        for a in range(per):
            comp[c, j, a, 0, rows, :] = re[j * per + a]
            comp[c, j, a, 1, rows, :] = im[j * per + a]


def doppler_chunk(recv, c, g, table, pw, hi_ref, lo_ref):
    quarter = recv.shape[3] // RADIX
    a, b, cc, d = ([recv[c, g, ri, q * quarter:(q + 1) * quarter, :] for ri in range(2)] for q in range(RADIX))
    sr, si = a[0] + cc[0], a[1] + cc[1]
    dr, di = a[0] - cc[0], a[1] - cc[1]
    ur, ui = b[0] + d[0], b[1] + d[1]
    vr, vi = b[0] - d[0], b[1] - d[1]
    ys = [(sr + ur, si + ui), (dr + vi, di - vr), (sr - ur, si - ui), (dr - vi, di + vr)]
    for res in range(RADIX):
        y = jnp.concatenate(ys[res], axis=0)
        near = y.astype(jnp.bfloat16)
        both = jnp.concatenate([near, (y - near.astype(jnp.float32)).astype(jnp.bfloat16)], axis=1)
        width = y.shape[0]
        main = jnp.dot(table[res, :, :width], both, preferred_element_type=jnp.float32)
        rest = jnp.dot(table[res, :, width:], near, preferred_element_type=jnp.float32)
        out = main[:, :LANES] + main[:, LANES:] + rest
        re, im = out[:quarter], out[quarter:]
        p = re * re + im * im
        hi = p.astype(jnp.bfloat16)
        pw[c, g, res] = p
        hi_ref[c, g + 1, res] = hi
        lo_ref[c, g + 1, res] = (p - hi.astype(jnp.float32)).astype(jnp.bfloat16)


def cfar_chunk(c, g, first_gate, gates, thresh, window, pw, hi_ref, lo_ref, band, acc):
    quarter = pw.shape[3]
    total = RADIX * quarter
    parts = [ref[c, g + k].reshape(total, LANES) for ref in (hi_ref, lo_ref) for k in range(3)]
    noise = jnp.dot(jnp.concatenate(parts, axis=1), band[c], preferred_element_type=jnp.float32)
    guard = window[c, 0]
    reach = guard + window[c, 1]
    gate = first_gate + g * LANES + lax.broadcasted_iota(jnp.int32, (SUB, LANES), 1)
    after = gates - 1 - gate
    cells = jnp.minimum(gate, reach) - jnp.minimum(gate, guard) + jnp.minimum(after, reach) - jnp.minimum(after, guard)
    cells = cells.astype(jnp.float32)[:1]
    inv = thresh[c, 1].astype(jnp.float32) / thresh[c, 0].astype(jnp.float32)
    ratio = pw[c, g].reshape(total, LANES) * cells / (noise + EPSILON)
    pw[c, g] = ratio.reshape(RADIX, quarter, LANES)
    soft = jnp.clip(ratio * inv - 1.0, 0.0, 1.0)
    acc[...] += jnp.sum(soft.reshape(total // SUB, SUB, LANES), axis=0)


def place_chunk(c, g, pw, stage, out):
    quarter = pw.shape[3]
    for res in range(RADIX):
        stage[pl.ds(res, quarter, stride=RADIX), :] = pw[c, g, res]
    out[c, :, pl.ds(pl.multiple_of(g * LANES, LANES), LANES)] = stage[...]


def kernel(sizes, rep_hbm, thresh_hbm, window_hbm, x_hbm, tw_hbm, wf_hbm, wi_hbm, t_hbm, out, count,
           rep, thresh, window, tw, nat, xs, wf, wi, table, tw8, rep8, comp, recv, pw, hi_ref, lo_ref, band, stage, pack, halo, gather, acc,
           in_sem, tab_sem, row_send, row_recv, chunk_send, chunk_recv, halo_send, halo_recv, sum_sem):
    n, nx, ns, rows = sizes
    _, channels, part, gates = xs.shape
    chunks = comp.shape[2]
    quarter = pw.shape[3]
    pulses = RADIX * quarter
    own = gates // n
    blocks = part // rows
    last = channels - 1
    z, x, s = lax.axis_index("pulse"), lax.axis_index("chan"), lax.axis_index("sub")
    peers = n * nx * ns
    me = (z * nx + x) * ns + s
    h = n // 2
    half = z // h

    def each(body, lo, hi):
        def run(i, carry):
            body(i)
            return carry
        lax.fori_loop(lo, hi, run, 0, unroll=hi - lo < 4)

    def beside(act):
        for ox in range(nx):
            for os in range(ns):
                if ox or os:
                    act({"pulse": z, "chan": lax.rem(x + ox, nx), "sub": lax.rem(s + os, ns)})

    def others(act):
        def along(o):
            for ox in range(nx):
                for os in range(ns):
                    act({"pulse": lax.rem(z + n - o, n), "chan": lax.rem(x + ox, nx), "sub": lax.rem(s + os, ns)})
        each(along, 1, n)
        beside(act)

    barrier = pltpu.get_barrier_semaphore()

    def load(b):
        c = b // blocks
        r = pl.ds(pl.multiple_of(lax.rem(b, blocks) * rows, rows), rows)
        return pltpu.make_async_copy(x_hbm.at[:, c, r, :], xs.at[:, c, r, :], in_sem.at[b])

    tables = [pltpu.make_async_copy(a, b, tab_sem.at[i])
              for i, (a, b) in enumerate(((rep_hbm, rep), (tw_hbm, tw), (wf_hbm, wf), (wi_hbm, wi), (t_hbm, table),
                                         (thresh_hbm, thresh), (window_hbm, window)))]
    tables[0].start()
    load(0).start()
    for copy in tables[1:4]:
        copy.start()
    def greet(who):
        pl.semaphore_signal(barrier, 1, device_id=who, device_id_type=MESH)

    each(lambda o: greet({"pulse": lax.rem(z + o, n)}), 1, n)
    beside(greet)
    for b in range(1, min(2, channels * blocks)):
        load(b).start()
    cols = tw.shape[1]
    nat[...] = jnp.zeros_like(nat)
    tables[0].wait()
    for ri in range(2):
        for k in range(cols):
            nat[ri * cols + k:ri * cols + k + 1, :] = rep[ri:ri + 1, k * LANES:(k + 1) * LANES]
    turned = jnp.transpose(nat[...])
    row = lax.broadcasted_iota(jnp.int32, (LANES, LANES), 0)
    lane = lax.broadcasted_iota(jnp.int32, (LANES, LANES), 1)
    per = LANES // cols
    pick = [jnp.where(jnp.logical_and(row >= ri * cols, lane == per * (row - ri * cols)), 1.0, 0.0) for ri in range(2)]
    pick = jnp.concatenate(pick, axis=1).astype(jnp.bfloat16)
    terms = []
    for _ in range(3):
        terms.append(turned.astype(jnp.bfloat16))
        turned = turned - terms[-1].astype(jnp.float32)
    placed = jnp.dot(jnp.concatenate(terms, axis=1), jnp.concatenate([pick] * 3, axis=0),
                     preferred_element_type=jnp.float32) * (INPUT_SCALE / gates)
    for ri in range(2):
        filt = placed[:cols, ri * LANES:(ri + 1) * LANES]
        for k in range(1, per):
            filt = filt + pltpu.roll(placed[k * cols:(k + 1) * cols, ri * LANES:(ri + 1) * LANES], k, 1)
        for k in range(cols):
            rep8[ri, k * SUB:(k + 1) * SUB, :] = jnp.broadcast_to(filt[k:k + 1, :], (SUB, LANES))
    tables[1].wait()
    for k in range(cols):
        for ri in range(2):
            tw8[ri, k * SUB:(k + 1) * SUB, :] = jnp.broadcast_to(tw[ri, k:k + 1, :], (SUB, LANES))

    def near(k):
        return half * h + lax.rem(lax.rem(z, h) + 1 + k, h)

    def cross(k):
        return (1 - half) * h + lax.rem(z + s + k, h)

    def row_copy(c, dest, b):
        r = pl.multiple_of(b * rows, rows)
        return pltpu.make_async_remote_copy(
            comp.at[c, dest, :, :, pl.ds(r, rows), :],
            recv.at[c, :, :, pl.ds(pl.multiple_of(z * part + r, rows), rows), :],
            row_send.at[c, dest], row_recv.at[c, z],
            device_id={"pulse": dest}, device_id_type=MESH)

    def row_all(c, dest, src):
        return pltpu.make_async_remote_copy(
            comp.at[c, dest], recv.at[c, :, :, pl.ds(pl.multiple_of(src * part, part), part), :],
            row_send.at[c, dest], row_recv.at[c, src],
            device_id={"pulse": dest}, device_id_type=MESH)

    def chunk_copy(dest, src, g):
        return pltpu.make_async_remote_copy(
            comp.at[last, dest, g], recv.at[last, g, :, pl.ds(pl.multiple_of(src * part, part), part), :],
            chunk_send.at[dest, g], chunk_recv.at[src, g],
            device_id={"pulse": dest}, device_id_type=MESH)

    outer = jnp.logical_and(n == 4, jnp.logical_or(z == 0, z == n - 1))

    def row_near(c, b):
        for k in range(h - 1):
            row_copy(c, near(k), b).start()

    def row_cross(c, b):
        for k in range(h):
            row_copy(c, cross(k), b).start()

    def step(b, carry):
        c = b // blocks
        r0 = lax.rem(b, blocks) * rows
        load(b).wait()

        @pl.when(b + 2 < channels * blocks)
        def _():
            load(b + 2).start()

        @pl.when(b == 0)
        def _():
            tables[2].wait()
            tables[3].wait()
            for copy in tables[4:]:
                copy.start()

        for u in range(rows // SUB):
            range_rows(xs, c, pl.multiple_of(r0 + u * SUB, SUB), tw8, rep8, wf, wi, comp)

        @pl.when(b == 0)
        def _():
            pl.semaphore_wait(barrier, n - 1 + nx * ns - 1)

        @pl.when(b < last * blocks)
        def _():
            pc, pb = c, lax.rem(b, blocks)

            @pl.when(outer)
            def _():
                row_near(pc, pb)

            @pl.when(jnp.logical_not(outer))
            def _():
                row_cross(pc, pb)

        return carry

    lax.fori_loop(0, channels * blocks, step, 0)

    def order(k):
        odd = lax.rem(k, 2)
        return odd * (chunks - 1) + (1 - 2 * odd) * (k // 2)

    def rest(t):
        c, b = t // blocks, lax.rem(t, blocks)

        @pl.when(outer)
        def _():
            row_cross(c, b)

        @pl.when(jnp.logical_not(outer))
        def _():
            row_near(c, b)

    def last_near(k):
        for q in range(h - 1):
            chunk_copy(near(q), z, order(k)).start()

    def far(q):
        return (1 - half) * (n - 1 - q) + half * q

    def last_cross(k):
        end = k // (chunks - 1) if chunks > 1 else 1
        for q in range(h):
            chunk_copy(end * far(q) + (1 - end) * cross(q), z, order(k)).start()

    ahead = min(AHEAD, chunks)
    each(last_near, 0, chunks)
    each(rest, 0, last * blocks)
    each(last_cross, 0, ahead)

    def keep(t):
        c, g = t // chunks, lax.rem(t, chunks)
        for ri in range(2):
            recv[c, g, ri, pl.ds(pl.multiple_of(z * part, part), part), :] = comp[c, z, g, ri]

    each(keep, 0, channels * chunks)
    for copy in tables[4:]:
        copy.wait()
    q = lax.broadcasted_iota(jnp.int32, (3 * LANES, LANES), 0)
    j = lax.broadcasted_iota(jnp.int32, (3 * LANES, LANES), 1)
    dist = jnp.abs(q - LANES - j)
    for c in range(channels):
        guard = window[c, 0]
        reach = guard + window[c, 1]
        inside = jnp.where(dist > guard, 1.0, 0.0) * jnp.where(dist <= reach, 1.0, 0.0)
        inside = inside.astype(jnp.bfloat16)
        band[c] = jnp.concatenate([inside, inside], axis=0)
        blank = jnp.zeros((RADIX, quarter, LANES), jnp.bfloat16)
        for ref in (hi_ref, lo_ref):
            ref[c, 0] = blank
            ref[c, chunks + 1] = blank
    acc[...] = jnp.zeros_like(acc)

    def dop(c, g):
        doppler_chunk(recv, c, g, table, pw, hi_ref, lo_ref)

    def rate(c, g):
        cfar_chunk(c, g, z * own, gates, thresh, window, pw, hi_ref, lo_ref, band, acc)

    def cfar(c, g):
        rate(c, g)
        place_chunk(c, g, pw, stage, out)

    def pack_left(c):
        pack[c, 0] = jnp.concatenate([pw[c, 0, res][:, :MARGIN] for res in range(RADIX)], axis=1)

    def pack_right(c):
        pack[c, 1] = jnp.concatenate([pw[c, chunks - 1, res][:, LANES - MARGIN:] for res in range(RADIX)], axis=1)

    def halo_copy(c, side, dest):
        return pltpu.make_async_remote_copy(
            pack.at[c, side], halo.at[c, 1 - side], halo_send.at[c, side], halo_recv.at[c, 1 - side],
            device_id={"pulse": dest}, device_id_type=MESH)

    def send_halo(c):
        @pl.when(z > 0)
        def _():
            halo_copy(c, 0, z - 1).start()

        @pl.when(z < n - 1)
        def _():
            halo_copy(c, 1, z + 1).start()

    def unpack(c, side):
        for res in range(RADIX):
            turn = (LANES - MARGIN - MARGIN * res if side == 0 else LANES - MARGIN * res) % LANES
            p = halo[c, side]
            if turn:
                p = pltpu.roll(p, turn, 1)
            hi = p.astype(jnp.bfloat16)
            at = 0 if side == 0 else chunks + 1
            hi_ref[c, at, res] = hi
            lo_ref[c, at, res] = (p - hi.astype(jnp.float32)).astype(jnp.bfloat16)

    def take_halo(c):
        @pl.when(z > 0)
        def _():
            halo_copy(c, 1, z).wait_recv()
            unpack(c, 0)

        @pl.when(z < n - 1)
        def _():
            halo_copy(c, 0, z).wait_recv()
            unpack(c, 1)

    for c in range(last):
        for o in range(1, n):
            row_all(c, z, lax.rem(z + o, n)).wait_recv()
        each(functools.partial(dop, c), 0, chunks)
        pack_left(c)
        pack_right(c)
        if chunks > 2:
            cfar(c, 1)
        send_halo(c)
        each(functools.partial(cfar, c), 2, chunks - 1)

    def arrive(k):
        for o in range(1, n):
            chunk_copy(z, lax.rem(z + o, n), order(k)).wait_recv()

    head = chunks - 1 if chunks >= 4 else chunks

    def last_step(k):
        @pl.when(k + ahead < chunks)
        def _():
            last_cross(k + ahead)

        arrive(k)
        dop(last, order(k))

        @pl.when(k == 0)
        def _():
            pack_left(last)

        @pl.when(k == min(1, chunks - 1))
        def _():
            pack_right(last)

        if chunks >= 4:
            @pl.when(k == 2)
            def _():
                send_halo(last)

            @pl.when(k >= 4)
            def _():
                cfar(last, order(k - 2))

    each(last_step, 0, head)
    if chunks < 4:
        send_halo(last)
        each(functools.partial(cfar, last), 1, chunks - 1)
    for c in range(channels):
        take_halo(c)
    edges = min(2, chunks)

    def edge(t):
        cfar(t // edges, lax.rem(t, edges) * (chunks - 1))

    each(edge, 0, channels * edges)
    if chunks >= 4:
        arrive(chunks - 1)
        dop(last, order(jnp.int32(chunks - 1)))
        for k in range(chunks - 3, chunks):
            rate(last, (k % 2) * (chunks - 1) + (1 - 2 * (k % 2)) * (k // 2))

    gather[me] = jnp.sum(acc[...], axis=0, keepdims=True)
    for c in range(channels):
        @pl.when(z > 0)
        def _():
            halo_copy(c, 0, z - 1).wait_send()

        @pl.when(z < n - 1)
        def _():
            halo_copy(c, 1, z + 1).wait_send()

    def tell(who):
        pltpu.make_async_remote_copy(
            gather.at[me], gather.at[me], sum_sem.at[0], sum_sem.at[1],
            device_id=who, device_id_type=MESH).start()

    others(tell)
    if chunks >= 4:
        each(lambda k: place_chunk(last, order(k), pw, stage, out), chunks - 3, chunks)
    for c in range(last):
        for o in range(1, n):
            row_all(c, lax.rem(z + o, n), z).wait_send()

    def sent(g):
        for o in range(1, n):
            chunk_copy(lax.rem(z + o, n), z, g).wait_send()

    each(sent, 0, chunks)
    every = pltpu.make_async_remote_copy(
        gather.at[pl.ds(0, peers - 1)], gather.at[pl.ds(0, peers - 1)], sum_sem.at[0], sum_sem.at[1],
        device_id={"pulse": lax.rem(z + 1, n)}, device_id_type=MESH)
    every.wait_recv()
    total = jnp.sum(gather[...], axis=0)
    total = jnp.sum(total, axis=1, keepdims=True) * (1024.0 / (pulses * gates))
    count[...] = jnp.broadcast_to(total, count.shape)
    every.wait_send()


def deliver_kernel(ratio, count, ratio_out, count_out, one, sem):
    channels, pulses, _ = ratio.shape
    step = pulses // 8
    copies = []
    for i in range(8 * channels):
        c, r = i // 8, pl.ds(i % 8 * step, step)
        copies.append(pltpu.make_async_copy(ratio.at[c, r], ratio_out.at[c, r], sem.at[i + 1]))
    for copy in copies:
        copy.start()
    one[0] = count[0, 0]
    copies.append(pltpu.make_async_copy(one, count_out, sem.at[0]))
    copies[-1].start()
    for copy in copies:
        copy.wait()


def deliver(ratio, count):
    return pl.pallas_call(
        deliver_kernel,
        in_specs=[pl.BlockSpec(memory_space=pltpu.VMEM)] * 2,
        out_specs=[pl.BlockSpec(memory_space=pltpu.HBM)] * 2,
        out_shape=[jax.ShapeDtypeStruct(ratio.shape, jnp.float32), jax.ShapeDtypeStruct((1,), jnp.float32)],
        scratch_shapes=[pltpu.SMEM((1,), jnp.float32), pltpu.SemaphoreType.DMA((8 * ratio.shape[0] + 1,))],
        compiler_params=pltpu.CompilerParams(vmem_limit_bytes=1 << 20),
    )(*(pltpu.with_memory_space_constraint(a, pltpu.VMEM) for a in (ratio, count)))


def local(samples, replica, window, thresh):
    _, channels, part, gates = samples.shape
    n, nx, ns = (lax.axis_size(a) for a in ("pulse", "chan", "sub"))
    cols = gates // LANES
    pulses = part * n
    own = gates // n
    chunks = own // LANES
    quarter = pulses // RADIX
    rows = min(ROWS, part)
    k1 = np.arange(cols)[:, None]
    b = np.arange(LANES)[None, :]
    ang = 2.0 * np.pi * ((k1 * b) % gates) / gates
    tw = np.stack([np.cos(ang), -np.sin(ang)]).astype(np.float32)
    wf, wi = lane_table(-1.0), lane_table(1.0)
    table = doppler_table(pulses)
    peers = n * nx * ns
    f32, bf16 = jnp.float32, jnp.bfloat16
    vmem, hbm = (pl.BlockSpec(memory_space=m) for m in (pltpu.VMEM, pltpu.HBM))
    dma = pltpu.SemaphoreType.DMA
    return deliver(*pl.pallas_call(
        functools.partial(kernel, (n, nx, ns, rows)),
        in_specs=[hbm] * 8,
        out_specs=[vmem, vmem],
        out_shape=[pltpu.VMEM((channels, pulses, own), f32), pltpu.VMEM((1, LANES), f32)],
        scratch_shapes=[
            pltpu.VMEM(replica.shape, f32),
            pltpu.SMEM(thresh.shape, jnp.int32),
            pltpu.SMEM(window.shape, jnp.int32),
            pltpu.VMEM(tw.shape, f32),
            pltpu.VMEM((LANES, LANES), f32),
            pltpu.VMEM((2, channels, part, gates), jnp.int32),
            pltpu.VMEM(wf.shape, bf16),
            pltpu.VMEM(wi.shape, bf16),
            pltpu.VMEM(table.shape, bf16),
            pltpu.VMEM((2, cols * SUB, LANES), f32),
            pltpu.VMEM((2, cols * SUB, LANES), f32),
            pltpu.VMEM((channels, n, chunks, 2, part, LANES), f32),
            pltpu.VMEM((channels, chunks, 2, pulses, LANES), f32),
            pltpu.VMEM((channels, chunks, RADIX, quarter, LANES), f32),
            pltpu.VMEM((channels, chunks + 2, RADIX, quarter, LANES), bf16),
            pltpu.VMEM((channels, chunks + 2, RADIX, quarter, LANES), bf16),
            pltpu.VMEM((channels, 6 * LANES, LANES), bf16),
            pltpu.VMEM((pulses, LANES), f32),
            pltpu.VMEM((channels, 2, quarter, LANES), f32),
            pltpu.VMEM((channels, 2, quarter, LANES), f32),
            pltpu.VMEM((peers, 1, LANES), f32),
            pltpu.VMEM((SUB, LANES), f32),
            dma((channels * (part // rows),)),
            dma((7,)),
            dma((channels, n)),
            dma((channels, n)),
            dma((n, chunks)),
            dma((n, chunks)),
            dma((channels, 2)),
            dma((channels, 2)),
            dma((2,)),
        ],
        compiler_params=pltpu.CompilerParams(
            collective_id=0, has_side_effects=True, vmem_limit_bytes=48 << 20),
        cost_estimate=pl.CostEstimate(flops=int(2e10), bytes_accessed=32 << 20, transcendentals=0),
    )(*(pltpu.with_memory_space_constraint(jnp.asarray(a), pltpu.HBM)
        for a in (replica, thresh, window, samples, tw, wf, wi, table))))


def solution(mesh):
    in_specs = (
        P(None, ("grp", "chan", "sub"), "pulse", None),
        P(),
        P(("grp", "chan", "sub"), None),
        P(("grp", "chan", "sub"), None),
    )
    out_specs = (P(("grp", "chan", "sub"), None, "pulse"), P("grp"))
    return jax.shard_map(lambda *a: tuple(local(*a)), mesh=mesh, in_specs=in_specs, out_specs=out_specs, check_vma=False)
```
